16 devices in a mesh: dp: 2 (over z), cp: 8 (over y, x, core).
Axes of the slice: x: 2, y: 2, z: 2, core: 2. Of those that a mesh axis runs over, the one named last changes fastest.
Arguments:
- x_in: bfloat16 [8, 1024, 3072], P('dp', 'cp'), parts along dimension 0
- dy_in: bfloat16 [8, 1024, 3072], P('dp', 'cp'), parts along dimension 0
- norm_gain: bfloat16 [3072], replicated
- w_q: bfloat16 [3072, 24, 128], replicated
- w_k: bfloat16 [3072, 8, 128], replicated
- w_v: bfloat16 [3072, 8, 128], replicated
- w_o: bfloat16 [24, 128, 3072], replicated
Outputs:
- output 1: bfloat16 [8, 1024, 3072], P('dp', 'cp'), parts along dimension 0
- output 2: bfloat16 [8, 1024, 3072], P('dp', 'cp'), parts along dimension 0
- output 3: float32 [6144], P('dp'), parts along dimension 0
- output 4: float32 [6144, 24, 128], P('dp'), parts along dimension 0
- output 5: float32 [6144, 8, 128], P('dp'), parts along dimension 0
- output 6: float32 [6144, 8, 128], P('dp'), parts along dimension 0
- output 7: float32 [48, 128, 3072], P('dp'), parts along dimension 0
There are 2 independent parts. The reference program is written for one: setup_inputs(seed, part) draws one part's arguments, and reference() takes and returns one part's arrays. A program takes and returns all parts, laid end to end along the dimension named above; an argument that names none is the same for every part.
All inputs are finite; a program needn't handle non-finite values.
Results may differ from the reference program's by a relative error of at most 0.00981.
Values are sent between devices in bfloat16 or wider.
A program may use at most 1 GiB of HBM per device.

```python
import jax
import jax.numpy as jnp
from jax import lax

BATCH_PART = 4
SEQ_LEN = 1024
BLOCK_LEN = 128
MODEL_DIM = 3072
Q_HEADS = 24
KV_HEADS = 8
HEAD_DIM = 128

N_BLOCKS = SEQ_LEN // BLOCK_LEN
GROUP_SIZE = Q_HEADS // KV_HEADS
SCALE = HEAD_DIM ** -0.5
EPS = 1e-6


def setup_inputs(seed: int = 0, part: int = 0) -> dict:
    part_keys = jax.random.split(jax.random.fold_in(jax.random.key(seed), part), 2)
    weight_keys = jax.random.split(jax.random.key(seed + 1), 5)
    act_shape = (BATCH_PART, SEQ_LEN, MODEL_DIM)
    x_in = jax.random.normal(part_keys[0], act_shape, jnp.float32)
    dy_in = jax.random.normal(part_keys[1], act_shape, jnp.float32)
    norm_gain = 1.0 + 0.25 * jax.random.normal(weight_keys[0], (MODEL_DIM,), jnp.float32)
    w_q = jax.random.normal(weight_keys[1], (MODEL_DIM, Q_HEADS, HEAD_DIM), jnp.float32) * MODEL_DIM ** -0.5
    w_k = jax.random.normal(weight_keys[2], (MODEL_DIM, KV_HEADS, HEAD_DIM), jnp.float32) * MODEL_DIM ** -0.5
    w_v = jax.random.normal(weight_keys[3], (MODEL_DIM, KV_HEADS, HEAD_DIM), jnp.float32) * MODEL_DIM ** -0.5
    w_o = jax.random.normal(weight_keys[4], (Q_HEADS, HEAD_DIM, MODEL_DIM), jnp.float32) * (Q_HEADS * HEAD_DIM) ** -0.5
    return {
        'x_in': x_in.astype(jnp.bfloat16),
        'dy_in': dy_in.astype(jnp.bfloat16),
        'norm_gain': norm_gain.astype(jnp.bfloat16),
        'w_q': w_q.astype(jnp.bfloat16),
        'w_k': w_k.astype(jnp.bfloat16),
        'w_v': w_v.astype(jnp.bfloat16),
        'w_o': w_o.astype(jnp.bfloat16),
    }


def reference(x_in, dy_in, norm_gain, w_q, w_k, w_v, w_o):
    x_f32 = x_in.astype(jnp.float32)
    inv_rms = lax.rsqrt(jnp.mean(x_f32 * x_f32, axis=-1, keepdims=True) + EPS)
    unit_x = x_f32 * inv_rms
    gain_f32 = norm_gain.astype(jnp.float32)
    x_norm = (unit_x * gain_f32).astype(jnp.bfloat16)
    flat_norm = x_norm.reshape(BATCH_PART * SEQ_LEN, MODEL_DIM)
    wq_flat = w_q.reshape(MODEL_DIM, Q_HEADS * HEAD_DIM)
    wk_flat = w_k.reshape(MODEL_DIM, KV_HEADS * HEAD_DIM)
    wv_flat = w_v.reshape(MODEL_DIM, KV_HEADS * HEAD_DIM)
    wo_flat = w_o.reshape(Q_HEADS * HEAD_DIM, MODEL_DIM)
    queries = jnp.dot(flat_norm, wq_flat, preferred_element_type=jnp.float32).astype(jnp.bfloat16)
    keys_all = jnp.dot(flat_norm, wk_flat, preferred_element_type=jnp.float32).astype(jnp.bfloat16)
    values_all = jnp.dot(flat_norm, wv_flat, preferred_element_type=jnp.float32).astype(jnp.bfloat16)
    keys_f32 = keys_all.reshape(BATCH_PART, SEQ_LEN, KV_HEADS, HEAD_DIM).astype(jnp.float32)
    values_f32 = values_all.reshape(BATCH_PART, SEQ_LEN, KV_HEADS, HEAD_DIM).astype(jnp.float32)
    q_blocks = queries.reshape(BATCH_PART, N_BLOCKS, BLOCK_LEN, KV_HEADS, GROUP_SIZE, HEAD_DIM).transpose(1, 0, 2, 3, 4, 5)
    key_pos = jnp.arange(SEQ_LEN)
    block_ids = jnp.arange(N_BLOCKS)

    def block_scores(q_blk, blk_id):
        scores = jnp.einsum('bqkgd,bskd->bkgqs', q_blk.astype(jnp.float32), keys_f32) * SCALE
        query_pos = blk_id * BLOCK_LEN + jnp.arange(BLOCK_LEN)
        visible = query_pos[:, None] >= key_pos[None, :]
        return scores, visible

    def forward_block(operands):
        q_blk, blk_id = operands
        scores, visible = block_scores(q_blk, blk_id)
        scores = jnp.where(visible, scores, -jnp.inf)
        row_max = jnp.max(scores, axis=-1)
        probs_raw = jnp.exp(scores - row_max[..., None])
        row_sum = jnp.sum(probs_raw, axis=-1)
        attn_blk = jnp.einsum('bkgqs,bskd->bkgqd', probs_raw.astype(jnp.bfloat16).astype(jnp.float32), values_f32) / row_sum[..., None]
        return attn_blk.astype(jnp.bfloat16), row_max + jnp.log(row_sum)

    attn_blocks, log_norm = lax.map(forward_block, (q_blocks, block_ids))
    attn_tok = attn_blocks.transpose(1, 0, 4, 2, 3, 5).reshape(BATCH_PART * SEQ_LEN, Q_HEADS * HEAD_DIM)
    proj_out = jnp.dot(attn_tok, wo_flat, preferred_element_type=jnp.float32)
    y_out = (x_f32 + proj_out.reshape(BATCH_PART, SEQ_LEN, MODEL_DIM)).astype(jnp.bfloat16)

    dy_flat = dy_in.reshape(BATCH_PART * SEQ_LEN, MODEL_DIM)
    d_wo = jnp.dot(attn_tok.T, dy_flat, preferred_element_type=jnp.float32).reshape(Q_HEADS, HEAD_DIM, MODEL_DIM)
    d_attn = jnp.dot(dy_flat, wo_flat.T, preferred_element_type=jnp.float32).astype(jnp.bfloat16)
    d_attn_blocks = d_attn.reshape(BATCH_PART, N_BLOCKS, BLOCK_LEN, KV_HEADS, GROUP_SIZE, HEAD_DIM).transpose(1, 0, 3, 4, 2, 5)
    delta_row = jnp.sum(d_attn_blocks.astype(jnp.float32) * attn_blocks.astype(jnp.float32), axis=-1)

    def backward_block(grad_carry, operands):
        d_keys, d_values = grad_carry
        q_blk, blk_id, d_attn_blk, delta_blk, log_blk = operands
        scores, visible = block_scores(q_blk, blk_id)
        probs_norm = jnp.where(visible, jnp.exp(scores - log_blk[..., None]), 0.0)
        d_attn_f32 = d_attn_blk.astype(jnp.float32)
        d_values = d_values + jnp.einsum('bkgqs,bkgqd->bskd', probs_norm.astype(jnp.bfloat16).astype(jnp.float32), d_attn_f32)
        d_probs = jnp.einsum('bkgqd,bskd->bkgqs', d_attn_f32, values_f32)
        d_scores = (probs_norm * (d_probs - delta_blk[..., None]) * SCALE).astype(jnp.bfloat16).astype(jnp.float32)
        d_query = jnp.einsum('bkgqs,bskd->bqkgd', d_scores, keys_f32)
        d_keys = d_keys + jnp.einsum('bkgqs,bqkgd->bskd', d_scores, q_blk.astype(jnp.float32))
        return (d_keys, d_values), d_query

    zero_kv = jnp.zeros((BATCH_PART, SEQ_LEN, KV_HEADS, HEAD_DIM), jnp.float32)
    grad_kv, d_query_blocks = lax.scan(backward_block, (zero_kv, zero_kv), (q_blocks, block_ids, d_attn_blocks, delta_row, log_norm))
    d_query = d_query_blocks.transpose(1, 0, 2, 3, 4, 5).reshape(BATCH_PART * SEQ_LEN, Q_HEADS * HEAD_DIM).astype(jnp.bfloat16)
    d_keys = grad_kv[0].reshape(BATCH_PART * SEQ_LEN, KV_HEADS * HEAD_DIM).astype(jnp.bfloat16)
    d_values = grad_kv[1].reshape(BATCH_PART * SEQ_LEN, KV_HEADS * HEAD_DIM).astype(jnp.bfloat16)
    d_wq = jnp.dot(flat_norm.T, d_query, preferred_element_type=jnp.float32).reshape(MODEL_DIM, Q_HEADS, HEAD_DIM)
    d_wk = jnp.dot(flat_norm.T, d_keys, preferred_element_type=jnp.float32).reshape(MODEL_DIM, KV_HEADS, HEAD_DIM)
    d_wv = jnp.dot(flat_norm.T, d_values, preferred_element_type=jnp.float32).reshape(MODEL_DIM, KV_HEADS, HEAD_DIM)
    d_norm = (jnp.dot(d_query, wq_flat.T, preferred_element_type=jnp.float32)
              + jnp.dot(d_keys, wk_flat.T, preferred_element_type=jnp.float32)
              + jnp.dot(d_values, wv_flat.T, preferred_element_type=jnp.float32)).reshape(BATCH_PART, SEQ_LEN, MODEL_DIM)
    d_gain = jnp.sum(d_norm * unit_x, axis=(0, 1))
    d_unit = d_norm * gain_f32
    d_x = inv_rms * (d_unit - unit_x * jnp.mean(d_unit * unit_x, axis=-1, keepdims=True))
    dx_out = (dy_in.astype(jnp.float32) + d_x).astype(jnp.bfloat16)
    return y_out, dx_out, d_gain, d_wq, d_wk, d_wv, d_wo
```

```python
import functools
import math

import jax
import jax.numpy as jnp
from jax import lax
from jax.experimental import pallas as pl
from jax.experimental.pallas import tpu as pltpu
from jax.sharding import PartitionSpec as P

EPS = 1e-6
HD = 128
LOG2E = math.log2(math.e)
NEG = -1e30
BIG = pltpu.CompilerParams(vmem_limit_bytes=60 * 1024 * 1024)


def dot(a, b, ca, cb):
    return lax.dot_general(a, b, (((ca,), (cb,)), ((), ())), preferred_element_type=jnp.float32)


def cost(flops, nbytes):
    return pl.CostEstimate(flops=int(flops), bytes_accessed=int(nbytes), transcendentals=0)


def relayout_kernel(core_ref, wq_ref, wk_ref, wv_ref, out_ref, half_ref, tmp):
    rows = wq_ref.shape[0]
    first = core_ref[0] == 0
    col, base = 0, 0
    for ref in (wq_ref, wk_ref, wv_ref):
        width = ref.shape[1] * HD
        start = col
        for g in range(ref.shape[1] // 8):
            tmp[...] = ref[:, 8 * g:8 * g + 8, :].astype(jnp.float32).reshape(rows * 8, HD)
            for h in range(8):
                out_ref[:, col:col + HD] = tmp[pl.ds(h, rows, stride=8), :].astype(jnp.bfloat16)
                col += HD
        half = width // 2
        half_ref[:, base:base + half] = jnp.where(first, out_ref[:, start:start + half], out_ref[:, start + half:start + width])
        base += half


def relayout(w_q, w_k, w_v, core):
    dm = w_q.shape[0]
    cols = (w_q.shape[1] + w_k.shape[1] + w_v.shape[1]) * HD
    rows = 256
    return pl.pallas_call(
        relayout_kernel,
        grid_spec=pltpu.PrefetchScalarGridSpec(
            num_scalar_prefetch=1, grid=(dm // rows,),
            in_specs=[pl.BlockSpec((rows, w.shape[1], HD), lambda i, c: (i, 0, 0)) for w in (w_q, w_k, w_v)],
            out_specs=[pl.BlockSpec((rows, cols), lambda i, c: (i, 0)), pl.BlockSpec((rows, cols // 2), lambda i, c: (i, 0))],
            scratch_shapes=[pltpu.VMEM((rows * 8, HD), jnp.float32)]),
        out_shape=[jax.ShapeDtypeStruct((dm, cols), jnp.bfloat16), jax.ShapeDtypeStruct((dm, cols // 2), jnp.bfloat16)],
        cost_estimate=cost(1e10, 4 * dm * cols), name='relayout')(core, w_q, w_k, w_v)


def near_kernel(cb, tbl_ref, a_ref, b_ref, w_ref, o_ref):
    m = pl.program_id(1)
    a = jnp.where(m == 0, a_ref[...], b_ref[...])
    o_ref[...] = dot(a, w_ref[...], 1, cb).astype(jnp.bfloat16)


def far_kernel(cb, tbl_ref, a_ref, w_ref, old_ref, o_ref):
    o_ref[...] = dot(a_ref[...], w_ref[...], 1, cb).astype(jnp.bfloat16)


def proj_specs(w, width, cb, row):
    bn = width // 2
    if cb == 0:
        return bn, pl.BlockSpec((w.shape[0], bn), lambda n, m, t: (0, n))
    return bn, pl.BlockSpec((bn, w.shape[1]), lambda n, m, t: (2 * t[row] + n, 0))


def proj_near(a, b, w, tbl, tok, width, cb, name):
    bm, dm = a.shape
    bn, w_spec = proj_specs(w, width, cb, 2)
    line = pl.BlockSpec((bm, dm), lambda n, m, t: (0, 0))
    return pl.pallas_call(
        functools.partial(near_kernel, cb),
        grid_spec=pltpu.PrefetchScalarGridSpec(
            num_scalar_prefetch=1, grid=(2, 2), in_specs=[line, line, w_spec],
            out_specs=pl.BlockSpec((bm, bn), lambda n, m, t: (t[m], n))),
        out_shape=jax.ShapeDtypeStruct((tok, width), jnp.bfloat16),
        compiler_params=BIG, cost_estimate=cost(4 * bm * dm * width, 2 * dm * width), name=name)(tbl, a, b, w)


def proj_far(a, w, old, tbl, bm, cb, name):
    tok, dm = a.shape
    width = old.shape[1]
    rest = tok // bm - 2
    bn, w_spec = proj_specs(w, width, cb, rest)
    return pl.pallas_call(
        functools.partial(far_kernel, cb),
        grid_spec=pltpu.PrefetchScalarGridSpec(
            num_scalar_prefetch=1, grid=(2, rest),
            in_specs=[pl.BlockSpec((bm, dm), lambda n, m, t: (t[m], 0)), w_spec, pl.BlockSpec(memory_space=pl.ANY)],
            out_specs=pl.BlockSpec((bm, bn), lambda n, m, t: (t[m], n))),
        out_shape=jax.ShapeDtypeStruct(old.shape, jnp.bfloat16), input_output_aliases={3: 0},
        compiler_params=BIG, cost_estimate=cost(2 * rest * bm * dm * width, 2 * tok * dm), name=name)(tbl, a, w, old)


def stack(ref, rb, nblk, rows, group):
    parts = [ref[rb * nblk:(rb + 1) * nblk, 0, :, g * HD:(g + 1) * HD].reshape(rows, HD) for g in range(group)]
    return jnp.concatenate(parts, axis=0)


def fwd_kernel(rows, q_ref, k_ref, v_ref, o_ref, l_ref):
    n, _, blk, width = q_ref.shape
    group, seq, nblk = width // HD, n * blk, rows // blk
    c2 = HD ** -0.5 * LOG2E
    k = k_ref[...].reshape(seq, HD)
    v = v_ref[...].reshape(seq, HD)
    tall = group * rows
    row = lax.broadcasted_iota(jnp.int32, (tall, rows), 0) % rows
    col = lax.broadcasted_iota(jnp.int32, (tall, rows), 1)
    visible = row >= col

    def score(rb):
        return dot(stack(q_ref, rb, nblk, rows, group), k[:(rb + 1) * rows], 1, 1)

    s_next = score(0)
    for rb in range(seq // rows):
        r0 = rb * rows
        s = s_next
        if rb + 1 < seq // rows:
            s_next = score(rb + 1)
        s_d = jnp.where(visible, s[:, r0:], NEG)
        m = jnp.max(s_d, axis=1, keepdims=True)
        if rb:
            m = jnp.maximum(m, jnp.max(s[:, :r0], axis=1, keepdims=True))
        m = m * c2
        p_d = jnp.exp2(s_d * c2 - m)
        l = jnp.sum(p_d, axis=1, keepdims=True)
        p = p_d.astype(jnp.bfloat16)
        if rb:
            p_o = jnp.exp2(s[:, :r0] * c2 - m)
            l = l + jnp.sum(p_o, axis=1, keepdims=True)
            p = jnp.concatenate([p_o.astype(jnp.bfloat16), p], axis=1)
        acc = dot(p, v[:r0 + rows], 1, 0)
        o = (acc / l).astype(jnp.bfloat16)
        log2n = jnp.broadcast_to(m + jnp.log2(l), (tall, 128))
        for g in range(group):
            for j in range(nblk):
                o_ref[rb * nblk + j, 0, :, g * HD:(g + 1) * HD] = o[g * rows + j * blk:g * rows + (j + 1) * blk]
            l_ref[0, g, :, r0:r0 + rows] = log2n[g * rows:(g + 1) * rows].T[0:1]


def attn_fwd(qkv, kvh, group):
    n, nb, s, _ = qkv.shape
    width = group * HD
    first = kvh * group
    return pl.pallas_call(
        functools.partial(fwd_kernel, 128), grid=(nb, kvh),
        in_specs=[pl.BlockSpec((n, 1, s, width), lambda b, h: (0, b, 0, h)),
                  pl.BlockSpec((n, 1, s, HD), lambda b, h: (0, b, 0, first + h)),
                  pl.BlockSpec((n, 1, s, HD), lambda b, h: (0, b, 0, first + kvh + h))],
        out_specs=[pl.BlockSpec((n, 1, s, width), lambda b, h: (0, b, 0, h)),
                   pl.BlockSpec((1, group, 1, n * s), lambda b, h: (b, h, 0, 0))],
        out_shape=[jax.ShapeDtypeStruct((n, nb, s, kvh * width), jnp.bfloat16),
                   jax.ShapeDtypeStruct((nb, kvh * group, 1, n * s), jnp.float32)],
        compiler_params=BIG, cost_estimate=cost(nb * kvh * group * 4 * (n * s) ** 2 * HD, 10 ** 7),
        name='attn_fwd')(qkv, qkv, qkv)


def bwd_kernel(rows, q_ref, k_ref, v_ref, o_ref, do_ref, l_ref, dq_ref, dk_ref, dv_ref, dq_acc):
    n, _, blk, width = q_ref.shape
    group, seq, nblk = width // HD, n * blk, rows // blk
    scale = HD ** -0.5
    c2 = scale * LOG2E
    k = k_ref[...].reshape(seq, HD)
    v = v_ref[...].reshape(seq, HD)
    row = lax.broadcasted_iota(jnp.int32, (rows, rows), 0)
    col = lax.broadcasted_iota(jnp.int32, (rows, rows), 1)
    visible = row <= col
    qs, dos, deltas = [], [], []
    for g in range(group):
        cols = slice(g * HD, (g + 1) * HD)
        qs.append(q_ref[:, 0, :, cols].reshape(seq, HD))
        d_o = do_ref[:, 0, :, cols].reshape(seq, HD)
        o = o_ref[:, 0, :, cols].reshape(seq, HD)
        dos.append(d_o)
        dcol = jnp.sum(d_o.astype(jnp.float32) * o.astype(jnp.float32), axis=1, keepdims=True)
        deltas.append(jnp.broadcast_to(dcol, (seq, 128)).T[0:1])
    units = [(kb, g) for kb in range(seq // rows) for g in range(group)]

    def score(unit):
        k0, g = unit[0] * rows, unit[1]
        return dot(k[k0:k0 + rows], qs[g][k0:], 1, 1), dot(v[k0:k0 + rows], dos[g][k0:], 1, 1)

    following = score(units[0])
    for i, (kb, g) in enumerate(units):
        k0 = kb * rows
        s, dp = following
        if i + 1 < len(units):
            following = score(units[i + 1])
        p = jnp.exp2(s * c2 - l_ref[0, g][:, k0:])
        p_d = jnp.where(visible, p[:, :rows], 0.0)
        p = p_d if k0 + rows == seq else jnp.concatenate([p_d, p[:, rows:]], axis=1)
        ds = (p * (dp - deltas[g][:, k0:]) * scale).astype(jnp.bfloat16)
        dv_c = dot(p.astype(jnp.bfloat16), dos[g][k0:], 1, 0)
        dk_c = dot(ds, qs[g][k0:], 1, 0)
        dq_c = dot(ds, k[k0:k0 + rows], 0, 0)
        if kb == 0:
            dq_acc[g] = dq_c
        else:
            dq_acc[g, k0:] += dq_c
        dv_t, dk_t = (dv_c, dk_c) if g == 0 else (dv_t + dv_c, dk_t + dk_c)
        if g == group - 1:
            dk_ref[kb * nblk:(kb + 1) * nblk, 0] = dk_t.astype(jnp.bfloat16).reshape(nblk, blk, HD)
            dv_ref[kb * nblk:(kb + 1) * nblk, 0] = dv_t.astype(jnp.bfloat16).reshape(nblk, blk, HD)
    for g in range(group):
        dq_ref[:, 0, :, g * HD:(g + 1) * HD] = dq_acc[g].astype(jnp.bfloat16).reshape(n, blk, HD)


def attn_bwd(qkv, o, do, log2n, kvh, group, h0, count):
    n, nb, s, _ = qkv.shape
    width = group * HD
    first = kvh * group
    q_in = pl.BlockSpec((n, 1, s, width), lambda b, h: (0, b, 0, h0 + h))
    q_out = pl.BlockSpec((n, 1, s, width), lambda b, h: (0, b, 0, h))
    k_out = pl.BlockSpec((n, 1, s, HD), lambda b, h: (0, b, 0, h))
    return pl.pallas_call(
        functools.partial(bwd_kernel, 256), grid=(nb, count),
        in_specs=[q_in,
                  pl.BlockSpec((n, 1, s, HD), lambda b, h: (0, b, 0, first + h0 + h)),
                  pl.BlockSpec((n, 1, s, HD), lambda b, h: (0, b, 0, first + kvh + h0 + h)),
                  q_in, q_in,
                  pl.BlockSpec((1, group, 1, n * s), lambda b, h: (b, h0 + h, 0, 0))],
        out_specs=[q_out, k_out, k_out],
        out_shape=[jax.ShapeDtypeStruct((n, nb, s, count * width), jnp.bfloat16),
                   jax.ShapeDtypeStruct((n, nb, s, count * HD), jnp.bfloat16),
                   jax.ShapeDtypeStruct((n, nb, s, count * HD), jnp.bfloat16)],
        scratch_shapes=[pltpu.VMEM((group, n * s, HD), jnp.float32)],
        compiler_params=BIG, cost_estimate=cost(nb * count * group * 10 * (n * s) ** 2 * HD, 10 ** 7),
        name='attn_bwd')(qkv, qkv, qkv, o, do, log2n)


def grad_wo_kernel(chip_ref, a_ref, b_ref, out_ref):
    out_ref[...] = dot(a_ref[...], b_ref[...], 0, 0)


def grad_wo(o, dy, chip, n_chips):
    tok, half = o.shape
    dm = dy.shape[1]
    bm, bn = half // n_chips, 1024
    return pl.pallas_call(
        grad_wo_kernel,
        grid_spec=pltpu.PrefetchScalarGridSpec(
            num_scalar_prefetch=1, grid=(dm // bn,),
            in_specs=[pl.BlockSpec((tok, bm), lambda n, c: (0, c[0])), pl.BlockSpec((tok, bn), lambda n, c: (0, n))],
            out_specs=pl.BlockSpec((bm, bn), lambda n, c: (0, n))),
        out_shape=jax.ShapeDtypeStruct((bm, dm), jnp.float32),
        compiler_params=BIG, cost_estimate=cost(2 * tok * bm * dm, 2 * tok * dm), name='grad_wo')(chip, o, dy)


def grad_wx_kernel(plan, n_src, n_out, core_ref, a_ref, *refs):
    srcs, fulls = refs[:2 * n_src], refs[2 * n_src:2 * n_src + n_out]
    sends, (buf, sem) = refs[2 * n_src + n_out:2 * n_src + 2 * n_out], refs[2 * n_src + 2 * n_out:]
    core = core_ref[0]
    n, nn = pl.program_id(1), pl.num_programs(1)
    step = pl.program_id(0) * nn + n

    def fetch(idx, slot):
        for pos, pieces in enumerate(plan):
            off = 0
            for half, which, lo, hi in pieces:
                for is_mine in (True, False):
                    src = srcs[2 * which + (0 if is_mine else 1)]

                    @pl.when(jnp.logical_and(idx == pos, (core == half) == is_mine))
                    def _(src=src, off=off, lo=lo, w=hi - lo):
                        pltpu.make_async_copy(src.at[:, pl.ds(lo, w)], buf.at[slot, :, pl.ds(off, w)], sem.at[slot]).start()
                off += hi - lo

    @pl.when(step == 0)
    def _():
        fetch(n, 0)

    @pl.when(step + 1 < pl.num_programs(0) * nn)
    def _():
        fetch(lax.rem(n + 1, nn), lax.rem(step + 1, 2))

    slot = lax.rem(step, 2)
    pltpu.make_async_copy(buf.at[slot], buf.at[slot], sem.at[slot]).wait()
    acc = dot(a_ref[...], buf[slot], 0, 0)
    rows = acc.shape[0]

    def store(refs):
        for ref in refs:
            flat = ref.reshape(rows * 8, HD)
            for h in range(8):
                flat[pl.ds(h, rows, stride=8), :] = acc[:, h * HD:(h + 1) * HD]

    if n_out == 1:
        store((fulls[0], sends[0]))
    else:
        for pos in range(n_out):
            @pl.when(n == pos)
            def _(pos=pos):
                store((fulls[pos], sends[pos]))


def grad_wx(x, srcs, plan, heads, core, name):
    tok, dm = x.shape
    bm = 768
    nm = dm // 2 // bm
    flat = [a for pair in srcs for a in pair]
    if len(heads) == 1:
        col = lambda n: n
    else:
        col = lambda n: 0
    return pl.pallas_call(
        functools.partial(grad_wx_kernel, plan, len(srcs), len(heads)),
        grid_spec=pltpu.PrefetchScalarGridSpec(
            num_scalar_prefetch=1, grid=(nm, len(plan)),
            in_specs=[pl.BlockSpec((tok, bm), lambda m, n, c: (0, c[0] * nm + m))]
            + [pl.BlockSpec(memory_space=pl.ANY)] * len(flat),
            out_specs=[pl.BlockSpec((bm, 8, HD), lambda m, n, c: (c[0] * nm + m, col(n), 0)) for _ in heads]
            + [pl.BlockSpec((bm, 8, HD), lambda m, n, c: (m, col(n), 0)) for _ in heads],
            scratch_shapes=[pltpu.VMEM((2, tok, 8 * HD), jnp.bfloat16), pltpu.SemaphoreType.DMA((2,))]),
        out_shape=[jax.ShapeDtypeStruct((dm, h, HD), jnp.float32) for h in heads]
        + [jax.ShapeDtypeStruct((dm // 2, h, HD), jnp.float32) for h in heads],
        compiler_params=BIG, cost_estimate=cost(tok * dm * 8 * HD * len(plan), 2 * tok * dm), name=name)(core, x, *flat)


def merge_kernel(core_ref, *refs):
    n = len(refs) // 3
    for i in range(n):
        refs[2 * n + i][...] = refs[n + i][...]


def merge(fulls, recvs, core):
    steps = 12
    n = len(fulls)

    def spec(a, mine):
        block = (a.shape[0] // steps,) + a.shape[1:]
        zeros = (0,) * (len(block) - 1)
        if mine:
            return pl.BlockSpec(block, lambda i, c: (i,) + zeros)
        return pl.BlockSpec(block, lambda i, c: ((1 - c[0]) * steps + i,) + zeros)

    return pl.pallas_call(
        merge_kernel,
        grid_spec=pltpu.PrefetchScalarGridSpec(
            num_scalar_prefetch=1, grid=(steps,),
            in_specs=[pl.BlockSpec(memory_space=pl.ANY)] * n + [spec(r, True) for r in recvs],
            out_specs=[spec(r, False) for r in recvs]),
        out_shape=[jax.ShapeDtypeStruct(f.shape, f.dtype) for f in fulls],
        input_output_aliases={1 + i: i for i in range(n)},
        cost_estimate=cost(1e10, 10 ** 8), name='merge')(core, *fulls, *recvs)


def y_kernel(idx_ref, loc_ref, rem_ref, w_ref, x_ref, y_ref, acc):
    k = pl.program_id(0)
    per = pl.num_programs(0) // 2
    nb, s, dm = x_ref.shape
    tok = nb * s
    mine = k // per == idx_ref[0]
    part = dot(jnp.where(mine, loc_ref[...].reshape(tok, -1), rem_ref[...].reshape(tok, -1)), w_ref[...], 1, 0)

    @pl.when(k == 0)
    def _():
        acc[...] = part

    @pl.when(k > 0)
    def _():
        acc[...] += part

    @pl.when(k == 2 * per - 1)
    def _():
        for b in range(nb):
            y_ref[b] = (x_ref[b].astype(jnp.float32) + acc[b * s:(b + 1) * s]).astype(jnp.bfloat16)


def out_proj(idx, o, o_rem, wo, x):
    nb, s, dm = x.shape
    wide = 768
    per = o.shape[3] // wide
    whole = pl.BlockSpec((nb, s, dm), lambda k, i: (0, 0, 0))
    return pl.pallas_call(
        y_kernel,
        grid_spec=pltpu.PrefetchScalarGridSpec(
            num_scalar_prefetch=1, grid=(2 * per,),
            in_specs=[pl.BlockSpec((1, nb, s, wide), lambda k, i: (i[1], 0, 0, lax.rem(k, per))),
                      pl.BlockSpec((nb, s, wide), lambda k, i: (0, 0, lax.rem(k, per))),
                      pl.BlockSpec((wide, dm), lambda k, i: (k, 0)), whole],
            out_specs=whole, scratch_shapes=[pltpu.VMEM((nb * s, dm), jnp.float32)]),
        out_shape=jax.ShapeDtypeStruct(x.shape, jnp.bfloat16),
        compiler_params=BIG, cost_estimate=cost(2 * nb * s * dm * dm, 2 * dm * dm), name='out_proj')(idx, o, o_rem, wo, x)


def dx_kernel(plan, n_src, idx_ref, *refs):
    srcs = refs[:2 * n_src]
    w_ref, x_ref, dy_ref, g_ref, dx_ref, dg_ref, acc = refs[2 * n_src:]
    k = pl.program_id(0)
    nb, s, dm = x_ref.shape
    for pos, pieces in enumerate(plan):
        @pl.when(k == pos)
        def _(pos=pos, pieces=pieces):
            cols = []
            for half, which, lo, hi in pieces:
                loc, rem = srcs[2 * which], srcs[2 * which + 1]
                cols.append(jnp.where(idx_ref[0] == half, loc[0, :, :, lo:hi].reshape(nb * s, hi - lo),
                                      rem[0, :, :, lo:hi].reshape(nb * s, hi - lo)))
            part = dot(jnp.concatenate(cols, axis=1), w_ref[...], 1, 1)
            if pos == 0:
                acc[...] = part
            else:
                acc[...] += part

    @pl.when(k == len(plan) - 1)
    def _():
        gain = g_ref[...].astype(jnp.float32)
        total = jnp.zeros((1, dm), jnp.float32)
        for b in range(nb):
            x32 = x_ref[b].astype(jnp.float32)
            inv = lax.rsqrt(jnp.mean(x32 * x32, axis=-1, keepdims=True) + EPS)
            unit = x32 * inv
            d_norm = acc[b * s:(b + 1) * s]
            total = total + jnp.sum(d_norm * unit, axis=0, keepdims=True)
            e = d_norm * gain
            d_x = inv * (e - unit * jnp.mean(e * unit, axis=-1, keepdims=True))
            dx_ref[b] = (dy_ref[b].astype(jnp.float32) + d_x).astype(jnp.bfloat16)
        dg_ref[...] = total


def cut(order, srcs, wide):
    plan, room = [], 0
    for half, which in order:
        lo, end = 0, srcs[which][0].shape[3]
        while lo < end:
            if room == 0:
                plan.append([])
                room = wide
            hi = min(end, lo + room)
            plan[-1].append((half, which, lo, hi))
            room -= hi - lo
            lo = hi
    return plan


def grad_x(idx, srcs, plan, wide, wcat, x, dy, gain):
    nb, s, dm = x.shape
    flat = [a for pair in srcs for a in pair]
    whole = pl.BlockSpec((nb, s, dm), lambda k, i: (0, 0, 0))
    line = pl.BlockSpec((1, dm), lambda k, i: (0, 0))
    return pl.pallas_call(
        functools.partial(dx_kernel, plan, len(srcs)),
        grid_spec=pltpu.PrefetchScalarGridSpec(
            num_scalar_prefetch=1, grid=(len(plan),),
            in_specs=[pl.BlockSpec((1, nb, s, a.shape[3]), lambda k, i: (i[1], 0, 0, 0)) for a in flat]
            + [pl.BlockSpec((dm, wide), lambda k, i: (0, k)), whole, whole, line],
            out_specs=[whole, line], scratch_shapes=[pltpu.VMEM((nb * s, dm), jnp.float32)]),
        out_shape=[jax.ShapeDtypeStruct(x.shape, jnp.bfloat16), jax.ShapeDtypeStruct((1, dm), jnp.float32)],
        compiler_params=BIG, cost_estimate=cost(2 * nb * s * dm * wide * len(plan), 2 * dm * dm),
        name='grad_x')(idx, *flat, wcat, x, dy, gain)


def solution(mesh):
    n_dev = mesh.shape['cp']
    n_chips = n_dev // 2
    pair = [(d, d ^ 1) for d in range(n_dev)]
    by_core = [[2 * p + c for c in range(2) for p in range(n_chips)]]

    def device_fn(x_in, dy_in, norm_gain, w_q, w_k, w_v, w_o):
        me = lax.axis_index('cp')
        core = me % 2
        nb, s, dm = x_in.shape
        n_heads, kv_heads = w_q.shape[1], w_k.shape[1]
        group = n_heads // kv_heads
        kvh = kv_heads // 2
        qd = n_heads * HD
        tok = n_dev * nb * s
        core_arr = core[None].astype(jnp.int32)
        chip_arr = (me // 2)[None].astype(jnp.int32)
        idx = jnp.stack([core, me]).astype(jnp.int32)

        def swap(a):
            return lax.ppermute(a, 'cp', pair)

        x32 = x_in.astype(jnp.float32)
        inv = lax.rsqrt(jnp.mean(x32 * x32, axis=-1, keepdims=True) + EPS)
        xn = (x32 * inv * norm_gain.astype(jnp.float32)).astype(jnp.bfloat16)
        own = nb * s
        xn = xn.reshape(own, dm)
        dy = dy_in.reshape(own, dm)
        xg = lax.all_gather(xn, 'cp', tiled=True)
        dyg = lax.all_gather(dy, 'cp', tiled=True)
        wcat, wh = relayout(w_q, w_k, w_v, core_arr)
        wo = w_o.reshape(qd, dm)
        near = jnp.stack([me, me ^ 1, core]).astype(jnp.int32)
        chip = me // 2
        far = [2 * lax.rem(chip + 1 + j // 2, n_chips) + j % 2 for j in range(n_dev - 2)]
        far = jnp.stack(far + [core]).astype(jnp.int32)
        qkv = proj_near(xn, swap(xn), wh, near, tok, wh.shape[1], 0, 'near_qkv')
        do = proj_near(dy, swap(dy), wo, near, tok, qd // 2, 1, 'near_do')
        qkv = proj_far(xg, wh, qkv, far, own, 0, 'far_qkv').reshape(n_dev, nb, s, -1)
        o, log2n = attn_fwd(qkv, kvh, group)
        dyg, o = lax.optimization_barrier((dyg, o))
        d_wo = lax.all_gather(grad_wo(o.reshape(tok, -1), dyg, chip_arr, n_chips), 'cp', axis_index_groups=by_core, tiled=True)
        do = proj_far(dyg, wo, do, far, own, 1, 'far_do').reshape(n_dev, nb, s, -1)
        o_rem = swap(lax.dynamic_index_in_dim(o, me ^ 1, 0, keepdims=False))
        half = kvh // 2
        first = attn_bwd(qkv, o, do, log2n, kvh, group, 0, half)
        first_rem = [swap(a) for a in first]
        second = attn_bwd(qkv, o, do, log2n, kvh, group, half, half)
        second_rem = [swap(a) for a in second]
        o_late, _ = lax.optimization_barrier((o, second[0]))
        y_out = out_proj(idx, o_late, o_rem, wo, x_in)
        rems, xg, y_out = lax.optimization_barrier((first_rem + second_rem, xg, y_out))
        pairs = list(zip(list(first) + list(second), rems))
        flat = [(a.reshape(tok, -1), b.reshape(tok, -1)) for a, b in pairs]
        wide = kv_heads * HD
        by_q = [(h, j) for h in range(2) for j in (0, 3)]
        by_k = [(h, j) for h in range(2) for j in (1, 4)]
        by_v = [(h, j) for h in range(2) for j in (2, 5)]
        wq_full, wq_send = grad_wx(xg, flat, cut(by_q, pairs, wide), (n_heads,), core_arr, 'grad_wq')
        wq_send, xg = lax.optimization_barrier((wq_send, xg))
        wq_recv = swap(wq_send)
        wk_full, wv_full, wk_send, wv_send = grad_wx(
            xg, flat, cut(by_k, pairs, wide) + cut(by_v, pairs, wide), (kv_heads, kv_heads), core_arr, 'grad_wkv')
        wk_send, wv_send, x_late = lax.optimization_barrier((wk_send, wv_send, x_in))
        wk_recv, wv_recv = swap(wk_send), swap(wv_send)
        dx_out, d_gain = grad_x(idx, pairs, cut(by_q + by_k + by_v, pairs, wide), wide, wcat, x_late, dy_in, norm_gain[None])
        d_gain = d_gain[0]
        for bit in (1, 2, 4):
            d_gain = d_gain + lax.ppermute(d_gain, 'cp', [(d, d ^ bit) for d in range(n_dev)])
        wq_recv, wk_recv, wv_recv, dx_out = lax.optimization_barrier((wq_recv, wk_recv, wv_recv, dx_out))
        d_wq, d_wk, d_wv = merge((wq_full, wk_full, wv_full), (wq_recv, wk_recv, wv_recv), core_arr)
        d_wo = d_wo.reshape(n_heads, HD, dm)
        return y_out, dx_out, d_gain, d_wq, d_wk, d_wv, d_wo

    act_spec = P('dp', 'cp', None)
    mat_spec = P(None, None, None)
    grad_spec = P('dp', None, None)
    return jax.shard_map(device_fn, mesh=mesh,
                         in_specs=(act_spec, act_spec, P(None), mat_spec, mat_spec, mat_spec, mat_spec),
                         out_specs=(act_spec, act_spec, P('dp'), grad_spec, grad_spec, grad_spec, grad_spec),
                         check_vma=False)
```

```python
import functools
import math

import jax
import jax.numpy as jnp
from jax import lax
from jax.experimental import pallas as pl
from jax.experimental.pallas import tpu as pltpu
from jax.sharding import PartitionSpec as P

EPS = 1e-6
HD = 128
LOG2E = math.log2(math.e)
NEG = -1e30
BIG = pltpu.CompilerParams(vmem_limit_bytes=60 * 1024 * 1024)


def dot(a, b, ca, cb):
    return lax.dot_general(a, b, (((ca,), (cb,)), ((), ())), preferred_element_type=jnp.float32)


def cost(flops, nbytes):
    return pl.CostEstimate(flops=int(flops), bytes_accessed=int(nbytes), transcendentals=0)


def relayout_kernel(core_ref, wq_ref, wk_ref, wv_ref, out_ref, half_ref, tmp):
    rows = wq_ref.shape[0]
    first = core_ref[0] == 0
    col, base = 0, 0
    for ref in (wq_ref, wk_ref, wv_ref):
        width = ref.shape[1] * HD
        start = col
        for g in range(ref.shape[1] // 8):
            tmp[...] = ref[:, 8 * g:8 * g + 8, :].astype(jnp.float32).reshape(rows * 8, HD)
            for h in range(8):
                out_ref[:, col:col + HD] = tmp[pl.ds(h, rows, stride=8), :].astype(jnp.bfloat16)
                col += HD
        half = width // 2
        half_ref[:, base:base + half] = jnp.where(first, out_ref[:, start:start + half], out_ref[:, start + half:start + width])
        base += half


def relayout(w_q, w_k, w_v, core):
    dm = w_q.shape[0]
    cols = (w_q.shape[1] + w_k.shape[1] + w_v.shape[1]) * HD
    rows = 256
    return pl.pallas_call(
        relayout_kernel,
        grid_spec=pltpu.PrefetchScalarGridSpec(
            num_scalar_prefetch=1, grid=(dm // rows,),
            in_specs=[pl.BlockSpec((rows, w.shape[1], HD), lambda i, c: (i, 0, 0)) for w in (w_q, w_k, w_v)],
            out_specs=[pl.BlockSpec((rows, cols), lambda i, c: (i, 0)), pl.BlockSpec((rows, cols // 2), lambda i, c: (i, 0))],
            scratch_shapes=[pltpu.VMEM((rows * 8, HD), jnp.float32)]),
        out_shape=[jax.ShapeDtypeStruct((dm, cols), jnp.bfloat16), jax.ShapeDtypeStruct((dm, cols // 2), jnp.bfloat16)],
        cost_estimate=cost(1e10, 4 * dm * cols), name='relayout')(core, w_q, w_k, w_v)


def near_kernel(cb, tbl_ref, a_ref, b_ref, w_ref, o_ref):
    m = pl.program_id(1)
    a = jnp.where(m == 0, a_ref[...], b_ref[...])
    o_ref[...] = dot(a, w_ref[...], 1, cb).astype(jnp.bfloat16)


def far_kernel(cb, tbl_ref, a_ref, w_ref, old_ref, o_ref):
    o_ref[...] = dot(a_ref[...], w_ref[...], 1, cb).astype(jnp.bfloat16)


def proj_specs(w, width, cb, row):
    bn = width // 2
    if cb == 0:
        return bn, pl.BlockSpec((w.shape[0], bn), lambda n, m, t: (0, n))
    return bn, pl.BlockSpec((bn, w.shape[1]), lambda n, m, t: (2 * t[row] + n, 0))


def proj_near(a, b, w, tbl, tok, width, cb, name):
    bm, dm = a.shape
    bn, w_spec = proj_specs(w, width, cb, 2)
    line = pl.BlockSpec((bm, dm), lambda n, m, t: (0, 0))
    return pl.pallas_call(
        functools.partial(near_kernel, cb),
        grid_spec=pltpu.PrefetchScalarGridSpec(
            num_scalar_prefetch=1, grid=(2, 2), in_specs=[line, line, w_spec],
            out_specs=pl.BlockSpec((bm, bn), lambda n, m, t: (t[m], n))),
        out_shape=jax.ShapeDtypeStruct((tok, width), jnp.bfloat16),
        compiler_params=BIG, cost_estimate=cost(4 * bm * dm * width, 2 * dm * width), name=name)(tbl, a, b, w)


def proj_far(a, w, old, tbl, bm, cb, name):
    tok, dm = a.shape
    width = old.shape[1]
    rest = tok // bm - 2
    bn, w_spec = proj_specs(w, width, cb, rest)
    return pl.pallas_call(
        functools.partial(far_kernel, cb),
        grid_spec=pltpu.PrefetchScalarGridSpec(
            num_scalar_prefetch=1, grid=(2, rest),
            in_specs=[pl.BlockSpec((bm, dm), lambda n, m, t: (t[m], 0)), w_spec, pl.BlockSpec(memory_space=pl.ANY)],
            out_specs=pl.BlockSpec((bm, bn), lambda n, m, t: (t[m], n))),
        out_shape=jax.ShapeDtypeStruct(old.shape, jnp.bfloat16), input_output_aliases={3: 0},
        compiler_params=BIG, cost_estimate=cost(2 * rest * bm * dm * width, 2 * tok * dm), name=name)(tbl, a, w, old)


def stack(ref, rb, nblk, rows, group):
    parts = [ref[rb * nblk:(rb + 1) * nblk, 0, :, g * HD:(g + 1) * HD].reshape(rows, HD) for g in range(group)]
    return jnp.concatenate(parts, axis=0)


def fwd_kernel(rows, q_ref, k_ref, v_ref, o_ref, l_ref):
    n, _, blk, width = q_ref.shape
    group, seq, nblk = width // HD, n * blk, rows // blk
    c2 = HD ** -0.5 * LOG2E
    k = k_ref[...].reshape(seq, HD)
    v = v_ref[...].reshape(seq, HD)
    tall = group * rows
    row = lax.broadcasted_iota(jnp.int32, (tall, rows), 0) % rows
    col = lax.broadcasted_iota(jnp.int32, (tall, rows), 1)
    visible = row >= col

    def score(rb):
        return dot(stack(q_ref, rb, nblk, rows, group), k[:(rb + 1) * rows], 1, 1)

    s_next = score(0)
    for rb in range(seq // rows):
        r0 = rb * rows
        s = s_next
        if rb + 1 < seq // rows:
            s_next = score(rb + 1)
        s_d = jnp.where(visible, s[:, r0:], NEG)
        m = jnp.max(s_d, axis=1, keepdims=True)
        if rb:
            m = jnp.maximum(m, jnp.max(s[:, :r0], axis=1, keepdims=True))
        m = m * c2
        p_d = jnp.exp2(s_d * c2 - m)
        l = jnp.sum(p_d, axis=1, keepdims=True)
        p = p_d.astype(jnp.bfloat16)
        if rb:
            p_o = jnp.exp2(s[:, :r0] * c2 - m)
            l = l + jnp.sum(p_o, axis=1, keepdims=True)
            p = jnp.concatenate([p_o.astype(jnp.bfloat16), p], axis=1)
        acc = dot(p, v[:r0 + rows], 1, 0)
        o = (acc / l).astype(jnp.bfloat16)
        log2n = jnp.broadcast_to(m + jnp.log2(l), (tall, 128))
        for g in range(group):
            for j in range(nblk):
                o_ref[rb * nblk + j, 0, :, g * HD:(g + 1) * HD] = o[g * rows + j * blk:g * rows + (j + 1) * blk]
            l_ref[0, g, :, r0:r0 + rows] = log2n[g * rows:(g + 1) * rows].T[0:1]


def attn_fwd(qkv, kvh, group):
    n, nb, s, _ = qkv.shape
    width = group * HD
    first = kvh * group
    return pl.pallas_call(
        functools.partial(fwd_kernel, 128), grid=(nb, kvh),
        in_specs=[pl.BlockSpec((n, 1, s, width), lambda b, h: (0, b, 0, h)),
                  pl.BlockSpec((n, 1, s, HD), lambda b, h: (0, b, 0, first + h)),
                  pl.BlockSpec((n, 1, s, HD), lambda b, h: (0, b, 0, first + kvh + h))],
        out_specs=[pl.BlockSpec((n, 1, s, width), lambda b, h: (0, b, 0, h)),
                   pl.BlockSpec((1, group, 1, n * s), lambda b, h: (b, h, 0, 0))],
        out_shape=[jax.ShapeDtypeStruct((n, nb, s, kvh * width), jnp.bfloat16),
                   jax.ShapeDtypeStruct((nb, kvh * group, 1, n * s), jnp.float32)],
        compiler_params=BIG, cost_estimate=cost(nb * kvh * group * 4 * (n * s) ** 2 * HD, 10 ** 7),
        name='attn_fwd')(qkv, qkv, qkv)


def bwd_kernel(rows, q_ref, k_ref, v_ref, o_ref, do_ref, l_ref, d_ref, dq_acc):
    n, _, blk, width = q_ref.shape
    group, seq, nblk = width // HD, n * blk, rows // blk
    scale = HD ** -0.5
    c2 = scale * LOG2E
    k = k_ref[...].reshape(seq, HD)
    v = v_ref[...].reshape(seq, HD)
    row = lax.broadcasted_iota(jnp.int32, (rows, rows), 0)
    col = lax.broadcasted_iota(jnp.int32, (rows, rows), 1)
    visible = row <= col
    qs, dos, deltas = [], [], []
    for g in range(group):
        cols = slice(g * HD, (g + 1) * HD)
        qs.append(q_ref[:, 0, :, cols].reshape(seq, HD))
        d_o = do_ref[:, 0, :, cols].reshape(seq, HD)
        o = o_ref[:, 0, :, cols].reshape(seq, HD)
        dos.append(d_o)
        dcol = jnp.sum(d_o.astype(jnp.float32) * o.astype(jnp.float32), axis=1, keepdims=True)
        deltas.append(jnp.broadcast_to(dcol, (seq, 128)).T[0:1])
    units = [(kb, g) for kb in range(seq // rows) for g in range(group)]

    def score(unit):
        k0, g = unit[0] * rows, unit[1]
        return dot(k[k0:k0 + rows], qs[g][k0:], 1, 1), dot(v[k0:k0 + rows], dos[g][k0:], 1, 1)

    following = score(units[0])
    for i, (kb, g) in enumerate(units):
        k0 = kb * rows
        s, dp = following
        if i + 1 < len(units):
            following = score(units[i + 1])
        p = jnp.exp2(s * c2 - l_ref[0, g][:, k0:])
        p_d = jnp.where(visible, p[:, :rows], 0.0)
        p = p_d if k0 + rows == seq else jnp.concatenate([p_d, p[:, rows:]], axis=1)
        ds = (p * (dp - deltas[g][:, k0:]) * scale).astype(jnp.bfloat16)
        dv_c = dot(p.astype(jnp.bfloat16), dos[g][k0:], 1, 0)
        dk_c = dot(ds, qs[g][k0:], 1, 0)
        dq_c = dot(ds, k[k0:k0 + rows], 0, 0)
        if kb == 0:
            dq_acc[g] = dq_c
        else:
            dq_acc[g, k0:] += dq_c
        dv_t, dk_t = (dv_c, dk_c) if g == 0 else (dv_t + dv_c, dk_t + dk_c)
        if g == group - 1:
            for j, total in enumerate((dk_t, dv_t)):
                cols = slice(width + j * HD, width + (j + 1) * HD)
                d_ref[kb * nblk:(kb + 1) * nblk, 0, :, cols] = total.astype(jnp.bfloat16).reshape(nblk, blk, HD)
    for g in range(group):
        d_ref[:, 0, :, g * HD:(g + 1) * HD] = dq_acc[g].astype(jnp.bfloat16).reshape(n, blk, HD)


def attn_bwd(qkv, o, do, log2n, kvh, group, h0, count):
    n, nb, s, _ = qkv.shape
    width = group * HD
    first = kvh * group
    q_in = pl.BlockSpec((n, 1, s, width), lambda b, h: (0, b, 0, h0 + h))
    out = width + 2 * HD
    return pl.pallas_call(
        functools.partial(bwd_kernel, 256), grid=(nb, count),
        in_specs=[q_in,
                  pl.BlockSpec((n, 1, s, HD), lambda b, h: (0, b, 0, first + h0 + h)),
                  pl.BlockSpec((n, 1, s, HD), lambda b, h: (0, b, 0, first + kvh + h0 + h)),
                  q_in, q_in,
                  pl.BlockSpec((1, group, 1, n * s), lambda b, h: (b, h0 + h, 0, 0))],
        out_specs=pl.BlockSpec((n, 1, s, out), lambda b, h: (0, b, 0, h)),
        out_shape=jax.ShapeDtypeStruct((n, nb, s, count * out), jnp.bfloat16),
        scratch_shapes=[pltpu.VMEM((group, n * s, HD), jnp.float32)],
        compiler_params=BIG, cost_estimate=cost(nb * count * group * 10 * (n * s) ** 2 * HD, 10 ** 7),
        name='attn_bwd')(qkv, qkv, qkv, o, do, log2n)


def grad_wo_kernel(chip_ref, a_ref, b_ref, out_ref):
    out_ref[...] = dot(a_ref[...], b_ref[...], 0, 0)


def grad_wo(o, dy, chip, n_chips):
    tok, half = o.shape
    dm = dy.shape[1]
    bm, bn = half // n_chips, 1024
    return pl.pallas_call(
        grad_wo_kernel,
        grid_spec=pltpu.PrefetchScalarGridSpec(
            num_scalar_prefetch=1, grid=(dm // bn,),
            in_specs=[pl.BlockSpec((tok, bm), lambda n, c: (0, c[0])), pl.BlockSpec((tok, bn), lambda n, c: (0, n))],
            out_specs=pl.BlockSpec((bm, bn), lambda n, c: (0, n))),
        out_shape=jax.ShapeDtypeStruct((bm, dm), jnp.float32),
        compiler_params=BIG, cost_estimate=cost(2 * tok * bm * dm, 2 * tok * dm), name='grad_wo')(chip, o, dy)


def grad_wx_kernel(plan, n_src, n_out, core_ref, a_ref, *refs):
    srcs, fulls = refs[:2 * n_src], refs[2 * n_src:2 * n_src + n_out]
    sends, (buf, sem) = refs[2 * n_src + n_out:2 * n_src + 2 * n_out], refs[2 * n_src + 2 * n_out:]
    core = core_ref[0]
    n, nn = pl.program_id(1), pl.num_programs(1)
    step = pl.program_id(0) * nn + n

    def fetch(idx, slot):
        for pos, pieces in enumerate(plan):
            off = 0
            for half, which, lo, hi in pieces:
                for is_mine in (True, False):
                    src = srcs[2 * which + (0 if is_mine else 1)]

                    @pl.when(jnp.logical_and(idx == pos, (core == half) == is_mine))
                    def _(src=src, off=off, lo=lo, w=hi - lo):
                        pltpu.make_async_copy(src.at[:, pl.ds(lo, w)], buf.at[slot, :, pl.ds(off, w)], sem.at[slot]).start()
                off += hi - lo

    @pl.when(step == 0)
    def _():
        fetch(n, 0)

    @pl.when(step + 1 < pl.num_programs(0) * nn)
    def _():
        fetch(lax.rem(n + 1, nn), lax.rem(step + 1, 2))

    slot = lax.rem(step, 2)
    pltpu.make_async_copy(buf.at[slot], buf.at[slot], sem.at[slot]).wait()
    acc = dot(a_ref[...], buf[slot], 0, 0)
    rows = acc.shape[0]

    def store(refs):
        for ref in refs:
            flat = ref.reshape(rows * 8, HD)
            for h in range(8):
                flat[pl.ds(h, rows, stride=8), :] = acc[:, h * HD:(h + 1) * HD]

    if n_out == 1:
        store((fulls[0], sends[0]))
    else:
        for pos in range(n_out):
            @pl.when(n == pos)
            def _(pos=pos):
                store((fulls[pos], sends[pos]))


def grad_wx(x, srcs, plan, heads, core, name):
    tok, dm = x.shape
    bm = 768
    nm = dm // 2 // bm
    flat = [a for pair in srcs for a in pair]
    if len(heads) == 1:
        col = lambda n: n
    else:
        col = lambda n: 0
    return pl.pallas_call(
        functools.partial(grad_wx_kernel, plan, len(srcs), len(heads)),
        grid_spec=pltpu.PrefetchScalarGridSpec(
            num_scalar_prefetch=1, grid=(nm, len(plan)),
            in_specs=[pl.BlockSpec((tok, bm), lambda m, n, c: (0, c[0] * nm + m))]
            + [pl.BlockSpec(memory_space=pl.ANY)] * len(flat),
            out_specs=[pl.BlockSpec((bm, 8, HD), lambda m, n, c: (c[0] * nm + m, col(n), 0)) for _ in heads]
            + [pl.BlockSpec((bm, 8, HD), lambda m, n, c: (m, col(n), 0)) for _ in heads],
            scratch_shapes=[pltpu.VMEM((2, tok, 8 * HD), jnp.bfloat16), pltpu.SemaphoreType.DMA((2,))]),
        out_shape=[jax.ShapeDtypeStruct((dm, h, HD), jnp.float32) for h in heads]
        + [jax.ShapeDtypeStruct((dm // 2, h, HD), jnp.float32) for h in heads],
        compiler_params=BIG, cost_estimate=cost(tok * dm * 8 * HD * len(plan), 2 * tok * dm), name=name)(core, x, *flat)


def merge_kernel(core_ref, *refs):
    n = (len(refs) - 2) // 3
    for i in range(n + 1):
        refs[2 * n + 1 + i][...] = refs[n + i][...]


def merge(fulls, recvs, gathered, core):
    steps = 12
    n = len(fulls)

    def spec(a, mine):
        block = (a.shape[0] // steps,) + a.shape[1:]
        zeros = (0,) * (len(block) - 1)
        if mine:
            return pl.BlockSpec(block, lambda i, c: (i,) + zeros)
        return pl.BlockSpec(block, lambda i, c: ((1 - c[0]) * steps + i,) + zeros)

    return pl.pallas_call(
        merge_kernel,
        grid_spec=pltpu.PrefetchScalarGridSpec(
            num_scalar_prefetch=1, grid=(steps,),
            in_specs=[pl.BlockSpec(memory_space=pl.ANY)] * n + [spec(r, True) for r in recvs] + [spec(gathered, True)],
            out_specs=[spec(r, False) for r in recvs] + [spec(gathered, True)]),
        out_shape=[jax.ShapeDtypeStruct(f.shape, f.dtype) for f in fulls] + [jax.ShapeDtypeStruct(gathered.shape, gathered.dtype)],
        input_output_aliases={1 + i: i for i in range(n)},
        compiler_params=BIG, cost_estimate=cost(1e10, 10 ** 8), name='merge')(core, *fulls, *recvs, gathered)


def y_kernel(idx_ref, loc_ref, rem_ref, w_ref, x_ref, y_ref, acc):
    k = pl.program_id(0)
    per = pl.num_programs(0) // 2
    nb, s, dm = x_ref.shape
    tok = nb * s
    mine = k // per == idx_ref[0]
    part = dot(jnp.where(mine, loc_ref[...].reshape(tok, -1), rem_ref[...].reshape(tok, -1)), w_ref[...], 1, 0)

    @pl.when(k == 0)
    def _():
        acc[...] = part

    @pl.when(k > 0)
    def _():
        acc[...] += part

    @pl.when(k == 2 * per - 1)
    def _():
        for b in range(nb):
            y_ref[b] = (x_ref[b].astype(jnp.float32) + acc[b * s:(b + 1) * s]).astype(jnp.bfloat16)


def out_proj(idx, o, o_rem, wo, x):
    nb, s, dm = x.shape
    wide = 768
    per = o.shape[3] // wide
    whole = pl.BlockSpec((nb, s, dm), lambda k, i: (0, 0, 0))
    return pl.pallas_call(
        y_kernel,
        grid_spec=pltpu.PrefetchScalarGridSpec(
            num_scalar_prefetch=1, grid=(2 * per,),
            in_specs=[pl.BlockSpec((1, nb, s, wide), lambda k, i: (i[1], 0, 0, lax.rem(k, per))),
                      pl.BlockSpec((nb, s, wide), lambda k, i: (0, 0, lax.rem(k, per))),
                      pl.BlockSpec((wide, dm), lambda k, i: (k, 0)), whole],
            out_specs=whole, scratch_shapes=[pltpu.VMEM((nb * s, dm), jnp.float32)]),
        out_shape=jax.ShapeDtypeStruct(x.shape, jnp.bfloat16),
        compiler_params=BIG, cost_estimate=cost(2 * nb * s * dm * dm, 2 * dm * dm), name='out_proj')(idx, o, o_rem, wo, x)


def dx_kernel(plan, n_src, idx_ref, *refs):
    srcs = refs[:2 * n_src]
    w_ref, x_ref, dy_ref, g_ref, dx_ref, dg_ref, acc = refs[2 * n_src:]
    k = pl.program_id(0)
    nb, s, dm = x_ref.shape
    for pos, pieces in enumerate(plan):
        @pl.when(k == pos)
        def _(pos=pos, pieces=pieces):
            cols = []
            for half, which, lo, hi in pieces:
                loc, rem = srcs[2 * which], srcs[2 * which + 1]
                cols.append(jnp.where(idx_ref[0] == half, loc[0, :, :, lo:hi].reshape(nb * s, hi - lo),
                                      rem[0, :, :, lo:hi].reshape(nb * s, hi - lo)))
            part = dot(jnp.concatenate(cols, axis=1), w_ref[...], 1, 1)
            if pos == 0:
                acc[...] = part
            else:
                acc[...] += part

    @pl.when(k == len(plan) - 1)
    def _():
        gain = g_ref[...].astype(jnp.float32)
        total = jnp.zeros((1, dm), jnp.float32)
        for b in range(nb):
            x32 = x_ref[b].astype(jnp.float32)
            inv = lax.rsqrt(jnp.mean(x32 * x32, axis=-1, keepdims=True) + EPS)
            unit = x32 * inv
            d_norm = acc[b * s:(b + 1) * s]
            total = total + jnp.sum(d_norm * unit, axis=0, keepdims=True)
            e = d_norm * gain
            d_x = inv * (e - unit * jnp.mean(e * unit, axis=-1, keepdims=True))
            dx_ref[b] = (dy_ref[b].astype(jnp.float32) + d_x).astype(jnp.bfloat16)
        dg_ref[...] = total


def cut(spans, wide):
    plan, room = [], 0
    for half, which, lo, end in spans:
        while lo < end:
            if room == 0:
                plan.append([])
                room = wide
            hi = min(end, lo + room)
            plan[-1].append((half, which, lo, hi))
            room -= hi - lo
            lo = hi
    return plan


def grad_x(idx, srcs, plan, wide, wcat, x, dy, gain):
    nb, s, dm = x.shape
    flat = [a for pair in srcs for a in pair]
    whole = pl.BlockSpec((nb, s, dm), lambda k, i: (0, 0, 0))
    line = pl.BlockSpec((1, dm), lambda k, i: (0, 0))
    return pl.pallas_call(
        functools.partial(dx_kernel, plan, len(srcs)),
        grid_spec=pltpu.PrefetchScalarGridSpec(
            num_scalar_prefetch=1, grid=(len(plan),),
            in_specs=[pl.BlockSpec((1, nb, s, a.shape[3]), lambda k, i: (i[1], 0, 0, 0)) for a in flat]
            + [pl.BlockSpec((dm, wide), lambda k, i: (0, k)), whole, whole, line],
            out_specs=[whole, line], scratch_shapes=[pltpu.VMEM((nb * s, dm), jnp.float32)]),
        out_shape=[jax.ShapeDtypeStruct(x.shape, jnp.bfloat16), jax.ShapeDtypeStruct((1, dm), jnp.float32)],
        compiler_params=BIG, cost_estimate=cost(2 * nb * s * dm * wide * len(plan), 2 * dm * dm),
        name='grad_x')(idx, *flat, wcat, x, dy, gain)


def solution(mesh):
    n_dev = mesh.shape['cp']
    n_chips = n_dev // 2
    pair = [(d, d ^ 1) for d in range(n_dev)]
    by_core = [[2 * p + c for c in range(2) for p in range(n_chips)]]

    def device_fn(x_in, dy_in, norm_gain, w_q, w_k, w_v, w_o):
        me = lax.axis_index('cp')
        core = me % 2
        nb, s, dm = x_in.shape
        n_heads, kv_heads = w_q.shape[1], w_k.shape[1]
        group = n_heads // kv_heads
        kvh = kv_heads // 2
        qd = n_heads * HD
        tok = n_dev * nb * s
        core_arr = core[None].astype(jnp.int32)
        chip_arr = (me // 2)[None].astype(jnp.int32)
        idx = jnp.stack([core, me]).astype(jnp.int32)

        def swap(a):
            return lax.ppermute(a, 'cp', pair)

        x32 = x_in.astype(jnp.float32)
        inv = lax.rsqrt(jnp.mean(x32 * x32, axis=-1, keepdims=True) + EPS)
        xn = (x32 * inv * norm_gain.astype(jnp.float32)).astype(jnp.bfloat16)
        own = nb * s
        xn = xn.reshape(own, dm)
        dy = dy_in.reshape(own, dm)
        xg = lax.all_gather(xn, 'cp', tiled=True)
        dyg = lax.all_gather(dy, 'cp', tiled=True)
        wcat, wh = relayout(w_q, w_k, w_v, core_arr)
        wo = w_o.reshape(qd, dm)
        near = jnp.stack([me, me ^ 1, core]).astype(jnp.int32)
        chip = me // 2
        far = [2 * lax.rem(chip + 1 + j // 2, n_chips) + j % 2 for j in range(n_dev - 2)]
        far = jnp.stack(far + [core]).astype(jnp.int32)
        qkv = proj_near(xn, swap(xn), wh, near, tok, wh.shape[1], 0, 'near_qkv')
        do = proj_near(dy, swap(dy), wo, near, tok, qd // 2, 1, 'near_do')
        qkv, do, xg = lax.optimization_barrier((qkv, do, xg))
        qkv = proj_far(xg, wh, qkv, far, own, 0, 'far_qkv').reshape(n_dev, nb, s, -1)
        o, log2n = attn_fwd(qkv, kvh, group)
        o_rem = swap(lax.dynamic_index_in_dim(o, me ^ 1, 0, keepdims=False))
        y_out = out_proj(idx, o, o_rem, wo, x_in)
        dyg, o, y_out = lax.optimization_barrier((dyg, o, y_out))
        d_wo = lax.all_gather(grad_wo(o.reshape(tok, -1), dyg, chip_arr, n_chips), 'cp', axis_index_groups=by_core, tiled=True)
        do = proj_far(dyg, wo, do, far, own, 1, 'far_do').reshape(n_dev, nb, s, -1)
        most = kvh - 1
        first = attn_bwd(qkv, o, do, log2n, kvh, group, 0, most)
        first_rem = swap(first)
        second = attn_bwd(qkv, o, do, log2n, kvh, group, most, kvh - most)
        second_rem = swap(second)
        first_rem, second_rem, xg = lax.optimization_barrier((first_rem, second_rem, xg))
        pairs = [(first, first_rem), (second, second_rem)]
        flat = [(a.reshape(tok, -1), b.reshape(tok, -1)) for a, b in pairs]
        wide = kv_heads * HD

        def columns(lo, hi):
            spans = []
            for h in range(2):
                for j in range(kvh):
                    base = (j % most) * (group + 2) * HD
                    spans.append((h, j // most, base + lo * HD, base + hi * HD))
            return spans

        by_q, by_k, by_v = columns(0, group), columns(group, group + 1), columns(group + 1, group + 2)
        wq_full, wq_send = grad_wx(xg, flat, cut(by_q, wide), (n_heads,), core_arr, 'grad_wq')
        wq_send, xg = lax.optimization_barrier((wq_send, xg))
        wq_recv = swap(wq_send)
        wk_full, wv_full, wk_send, wv_send = grad_wx(
            xg, flat, cut(by_k + by_v, wide), (kv_heads, kv_heads), core_arr, 'grad_wkv')
        wk_send, wv_send, x_late = lax.optimization_barrier((wk_send, wv_send, x_in))
        wk_recv, wv_recv = swap(wk_send), swap(wv_send)
        dx_out, d_gain = grad_x(idx, pairs, cut(by_q + by_k + by_v, wide), wide, wcat, x_late, dy_in, norm_gain[None])
        d_gain = d_gain[0]

        def add_from(bit, a):
            return a + lax.ppermute(a, 'cp', [(d, d ^ bit) for d in range(n_dev)])

        d_gain = add_from(2, add_from(1, d_gain))
        wq_recv, wk_recv, wv_recv, d_wo, dx_out = lax.optimization_barrier((wq_recv, wk_recv, wv_recv, d_wo, dx_out))
        d_wq, d_wk, d_wv, d_wo = merge((wq_full, wk_full, wv_full), (wq_recv, wk_recv, wv_recv), d_wo, core_arr)
        d_gain = add_from(4, d_gain)
        d_wo = d_wo.reshape(n_heads, HD, dm)
        return y_out, dx_out, d_gain, d_wq, d_wk, d_wv, d_wo

    act_spec = P('dp', 'cp', None)
    mat_spec = P(None, None, None)
    grad_spec = P('dp', None, None)
    return jax.shard_map(device_fn, mesh=mesh,
                         in_specs=(act_spec, act_spec, P(None), mat_spec, mat_spec, mat_spec, mat_spec),
                         out_specs=(act_spec, act_spec, P('dp'), grad_spec, grad_spec, grad_spec, grad_spec),
                         check_vma=False)
```

```python
import functools
import math

import jax
import jax.numpy as jnp
from jax import lax
from jax.experimental import pallas as pl
from jax.experimental.pallas import tpu as pltpu
from jax.sharding import PartitionSpec as P


EPS = 1e-6
HD = 128
LOG2E = math.log2(math.e)
NEG = -1e30
BIG = pltpu.CompilerParams(vmem_limit_bytes=60 * 1024 * 1024)


def dot(a, b, ca, cb):
    return lax.dot_general(a, b, (((ca,), (cb,)), ((), ())), preferred_element_type=jnp.float32)


def cost(flops, nbytes):
    return pl.CostEstimate(flops=int(flops), bytes_accessed=int(nbytes), transcendentals=0)


def relayout_kernel(core_ref, wq_ref, wk_ref, wv_ref, out_ref, half_ref, tmp):
    rows = wq_ref.shape[0]
    first = core_ref[0] == 0
    col, base = 0, 0
    for ref in (wq_ref, wk_ref, wv_ref):
        width = ref.shape[1] * HD
        start = col
        for g in range(ref.shape[1] // 8):
            tmp[...] = ref[:, 8 * g:8 * g + 8, :].astype(jnp.float32).reshape(rows * 8, HD)
            for h in range(8):
                out_ref[:, col:col + HD] = tmp[pl.ds(h, rows, stride=8), :].astype(jnp.bfloat16)
                col += HD
        half = width // 2
        half_ref[:, base:base + half] = jnp.where(first, out_ref[:, start:start + half], out_ref[:, start + half:start + width])
        base += half


def relayout(w_q, w_k, w_v, core):
    dm = w_q.shape[0]
    cols = (w_q.shape[1] + w_k.shape[1] + w_v.shape[1]) * HD
    rows = 256
    return pl.pallas_call(
        relayout_kernel,
        grid_spec=pltpu.PrefetchScalarGridSpec(
            num_scalar_prefetch=1, grid=(dm // rows,),
            in_specs=[pl.BlockSpec((rows, w.shape[1], HD), lambda i, c: (i, 0, 0)) for w in (w_q, w_k, w_v)],
            out_specs=[pl.BlockSpec((rows, cols), lambda i, c: (i, 0)), pl.BlockSpec((rows, cols // 2), lambda i, c: (i, 0))],
            scratch_shapes=[pltpu.VMEM((rows * 8, HD), jnp.float32)]),
        out_shape=[jax.ShapeDtypeStruct((dm, cols), jnp.bfloat16), jax.ShapeDtypeStruct((dm, cols // 2), jnp.bfloat16)],
        cost_estimate=cost(1e10, 4 * dm * cols), name='relayout')(core, w_q, w_k, w_v)


def proj_kernel(cb, counts, tbl_ref, *refs):
    n_in = sum(counts)
    w_ref, (o_ref, x_ref, buf, sem) = refs[n_in], refs[-4:]
    m, nm = pl.program_id(1), pl.num_programs(1)
    step = pl.program_id(0) * nm + m

    def fetch(idx, slot):
        at = 0
        for j, count in enumerate(counts):
            @pl.when(idx == j)
            def _(parts=refs[at:at + count]):
                row = 0
                for part in parts:
                    rows = part.shape[0]
                    pltpu.make_async_copy(part, buf.at[slot, pl.ds(row, rows)], sem.at[slot]).start()
                    row += rows

            at += count

    @pl.when(step == 0)
    def _():
        fetch(m, 0)

    @pl.when(step + 1 < pl.num_programs(0) * nm)
    def _():
        fetch(lax.rem(m + 1, nm), lax.rem(step + 1, 2))

    slot = lax.rem(step, 2)
    pltpu.make_async_copy(buf.at[slot], buf.at[slot], sem.at[slot]).wait()
    a = buf[slot]
    o_ref[...] = dot(a, w_ref[...], 1, cb).astype(jnp.bfloat16)
    x_ref[...] = a


def proj(pieces, w, blocks, core, tok, width, cb, old):
    dm = pieces[0][0].shape[1]
    bm = sum(p.shape[0] for p in pieces[0])
    bn = width // 2
    nm = len(pieces)
    tbl = jnp.stack(blocks + [core]).astype(jnp.int32)
    flat = [p for piece in pieces for p in piece]
    if cb == 0:
        w_spec = pl.BlockSpec((dm, bn), lambda n, m, t: (0, n))
    else:
        w_spec = pl.BlockSpec((bn, dm), lambda n, m, t: (2 * t[nm] + n, 0))
    any_spec = pl.BlockSpec(memory_space=pl.ANY)
    first = 2 + len(flat)
    return pl.pallas_call(
        functools.partial(proj_kernel, cb, [len(p) for p in pieces]),
        grid_spec=pltpu.PrefetchScalarGridSpec(
            num_scalar_prefetch=1, grid=(2, nm),
            in_specs=[any_spec] * len(flat) + [w_spec] + [any_spec] * len(old),
            out_specs=[pl.BlockSpec((bm, bn), lambda n, m, t: (t[m], n)), pl.BlockSpec((bm, dm), lambda n, m, t: (t[m], 0))],
            scratch_shapes=[pltpu.VMEM((2, bm, dm), jnp.bfloat16), pltpu.SemaphoreType.DMA((2,))]),
        out_shape=[jax.ShapeDtypeStruct((tok, width), jnp.bfloat16), jax.ShapeDtypeStruct((tok, dm), jnp.bfloat16)],
        input_output_aliases={first + i: i for i in range(len(old))},
        compiler_params=BIG, cost_estimate=cost(2 * nm * bm * dm * width, 2 * dm * width))(tbl, *flat, w, *old)


def stack(ref, rb, nblk, rows, group):
    parts = [ref[rb * nblk:(rb + 1) * nblk, 0, :, g * HD:(g + 1) * HD].reshape(rows, HD) for g in range(group)]
    return jnp.concatenate(parts, axis=0)


def fwd_kernel(rows, q_ref, k_ref, v_ref, *refs):
    o_ref, l_ref = refs[-2:]
    n, _, blk, width = q_ref.shape
    group, seq, nblk = width // HD, n * blk, rows // blk
    c2 = HD ** -0.5 * LOG2E
    k = k_ref[...].reshape(seq, HD)
    v = v_ref[...].reshape(seq, HD)
    tall = group * rows
    row = lax.broadcasted_iota(jnp.int32, (tall, rows), 0) % rows
    col = lax.broadcasted_iota(jnp.int32, (tall, rows), 1)
    visible = row >= col

    def score(rb):
        return dot(stack(q_ref, rb, nblk, rows, group), k[:(rb + 1) * rows], 1, 1)

    s_next = score(0)
    for rb in range(seq // rows):
        r0 = rb * rows
        s = s_next
        if rb + 1 < seq // rows:
            s_next = score(rb + 1)
        s_d = jnp.where(visible, s[:, r0:], NEG)
        m = jnp.max(s_d, axis=1, keepdims=True)
        if rb:
            m = jnp.maximum(m, jnp.max(s[:, :r0], axis=1, keepdims=True))
        m = m * c2
        p_d = jnp.exp2(s_d * c2 - m)
        l = jnp.sum(p_d, axis=1, keepdims=True)
        p = p_d.astype(jnp.bfloat16)
        if rb:
            p_o = jnp.exp2(s[:, :r0] * c2 - m)
            l = l + jnp.sum(p_o, axis=1, keepdims=True)
            p = jnp.concatenate([p_o.astype(jnp.bfloat16), p], axis=1)
        acc = dot(p, v[:r0 + rows], 1, 0)
        o = (acc / l).astype(jnp.bfloat16)
        log2n = jnp.broadcast_to(m + jnp.log2(l), (tall, 128))
        for g in range(group):
            for j in range(nblk):
                o_ref[rb * nblk + j, 0, :, g * HD:(g + 1) * HD] = o[g * rows + j * blk:g * rows + (j + 1) * blk]
            l_ref[0, g, :, r0:r0 + rows] = log2n[g * rows:(g + 1) * rows].T[0:1]


def attn_fwd(qkv, kvh, group, b0, count, old):
    n, nb, s, _ = qkv.shape
    width = group * HD
    first = kvh * group
    return pl.pallas_call(
        functools.partial(fwd_kernel, 128), grid=(count, kvh),
        in_specs=[pl.BlockSpec((n, 1, s, width), lambda b, h: (0, b0 + b, 0, h)),
                  pl.BlockSpec((n, 1, s, HD), lambda b, h: (0, b0 + b, 0, first + h)),
                  pl.BlockSpec((n, 1, s, HD), lambda b, h: (0, b0 + b, 0, first + kvh + h))]
        + [pl.BlockSpec(memory_space=pl.ANY)] * len(old),
        out_specs=[pl.BlockSpec((n, 1, s, width), lambda b, h: (0, b0 + b, 0, h)),
                   pl.BlockSpec((1, group, 1, n * s), lambda b, h: (b0 + b, h, 0, 0))],
        out_shape=[jax.ShapeDtypeStruct((n, nb, s, kvh * width), jnp.bfloat16),
                   jax.ShapeDtypeStruct((nb, kvh * group, 1, n * s), jnp.float32)],
        input_output_aliases={3 + i: i for i in range(len(old))},
        compiler_params=BIG, cost_estimate=cost(count * kvh * group * 4 * (n * s) ** 2 * HD, 10 ** 7),
        name='attn_fwd')(qkv, qkv, qkv, *old)


def bwd_kernel(rows, q_ref, k_ref, v_ref, o_ref, do_ref, l_ref, d_ref, dq_acc):
    n, _, blk, width = q_ref.shape
    group, seq, nblk = width // HD, n * blk, rows // blk
    scale = HD ** -0.5
    c2 = scale * LOG2E
    k = k_ref[...].reshape(seq, HD)
    v = v_ref[...].reshape(seq, HD)
    row = lax.broadcasted_iota(jnp.int32, (rows, rows), 0)
    col = lax.broadcasted_iota(jnp.int32, (rows, rows), 1)
    visible = row <= col
    qs, dos, deltas = [], [], []
    for g in range(group):
        cols = slice(g * HD, (g + 1) * HD)
        qs.append(q_ref[:, 0, :, cols].reshape(seq, HD))
        d_o = do_ref[:, 0, :, cols].reshape(seq, HD)
        o = o_ref[:, 0, :, cols].reshape(seq, HD)
        dos.append(d_o)
        dcol = jnp.sum(d_o.astype(jnp.float32) * o.astype(jnp.float32), axis=1, keepdims=True)
        deltas.append(jnp.broadcast_to(dcol, (seq, 128)).T[0:1])
    units = [(kb, g) for kb in range(seq // rows) for g in range(group)]

    def score(unit):
        k0, g = unit[0] * rows, unit[1]
        return dot(k[k0:k0 + rows], qs[g][k0:], 1, 1), dot(v[k0:k0 + rows], dos[g][k0:], 1, 1)

    following = score(units[0])
    for i, (kb, g) in enumerate(units):
        k0 = kb * rows
        s, dp = following
        if i + 1 < len(units):
            following = score(units[i + 1])
        p = jnp.exp2(s * c2 - l_ref[0, g][:, k0:])
        p_d = jnp.where(visible, p[:, :rows], 0.0)
        p = p_d if k0 + rows == seq else jnp.concatenate([p_d, p[:, rows:]], axis=1)
        ds = (p * (dp - deltas[g][:, k0:]) * scale).astype(jnp.bfloat16)
        dv_c = dot(p.astype(jnp.bfloat16), dos[g][k0:], 1, 0)
        dk_c = dot(ds, qs[g][k0:], 1, 0)
        dq_c = dot(ds, k[k0:k0 + rows], 0, 0)
        if kb == 0:
            dq_acc[g] = dq_c
        else:
            dq_acc[g, k0:] += dq_c
        dv_t, dk_t = (dv_c, dk_c) if g == 0 else (dv_t + dv_c, dk_t + dk_c)
        if g == group - 1:
            for j, total in enumerate((dk_t, dv_t)):
                cols = slice(width + j * HD, width + (j + 1) * HD)
                d_ref[kb * nblk:(kb + 1) * nblk, 0, :, cols] = total.astype(jnp.bfloat16).reshape(nblk, blk, HD)
    for g in range(group):
        d_ref[:, 0, :, g * HD:(g + 1) * HD] = dq_acc[g].astype(jnp.bfloat16).reshape(n, blk, HD)


def attn_bwd(qkv, o, do, log2n, kvh, group, h0, count):
    n, nb, s, _ = qkv.shape
    width = group * HD
    first = kvh * group
    q_in = pl.BlockSpec((n, 1, s, width), lambda b, h: (0, b, 0, h0 + h))
    out = width + 2 * HD
    return pl.pallas_call(
        functools.partial(bwd_kernel, 256), grid=(nb, count),
        in_specs=[q_in,
                  pl.BlockSpec((n, 1, s, HD), lambda b, h: (0, b, 0, first + h0 + h)),
                  pl.BlockSpec((n, 1, s, HD), lambda b, h: (0, b, 0, first + kvh + h0 + h)),
                  q_in, q_in,
                  pl.BlockSpec((1, group, 1, n * s), lambda b, h: (b, h0 + h, 0, 0))],
        out_specs=pl.BlockSpec((n, 1, s, out), lambda b, h: (0, b, 0, h)),
        out_shape=jax.ShapeDtypeStruct((n, nb, s, count * out), jnp.bfloat16),
        scratch_shapes=[pltpu.VMEM((group, n * s, HD), jnp.float32)],
        compiler_params=BIG, cost_estimate=cost(nb * count * group * 10 * (n * s) ** 2 * HD, 10 ** 7),
        name='attn_bwd')(qkv, qkv, qkv, o, do, log2n)


def grad_wo_kernel(chip_ref, a_ref, b_ref, out_ref):
    out_ref[...] = dot(a_ref[...], b_ref[...], 0, 0)


def grad_wo(o, dy, chip, n_chips):
    tok, half = o.shape
    dm = dy.shape[1]
    bm, bn = half // n_chips, 1024
    return pl.pallas_call(
        grad_wo_kernel,
        grid_spec=pltpu.PrefetchScalarGridSpec(
            num_scalar_prefetch=1, grid=(dm // bn,),
            in_specs=[pl.BlockSpec((tok, bm), lambda n, c: (0, c[0])), pl.BlockSpec((tok, bn), lambda n, c: (0, n))],
            out_specs=pl.BlockSpec((bm, bn), lambda n, c: (0, n))),
        out_shape=jax.ShapeDtypeStruct((bm, dm), jnp.float32),
        compiler_params=BIG, cost_estimate=cost(2 * tok * bm * dm, 2 * tok * dm), name='grad_wo')(chip, o, dy)


def grad_wx_kernel(plan, n_src, n_out, core_ref, a_ref, *refs):
    srcs, fulls = refs[:2 * n_src], refs[2 * n_src:2 * n_src + n_out]
    sends, (buf, sem) = refs[2 * n_src + n_out:2 * n_src + 2 * n_out], refs[2 * n_src + 2 * n_out:]
    core = core_ref[0]
    n, nn = pl.program_id(1), pl.num_programs(1)
    step = pl.program_id(0) * nn + n

    def fetch(idx, slot):
        for pos, pieces in enumerate(plan):
            off = 0
            for half, which, lo, hi in pieces:
                for is_mine in (True, False):
                    src = srcs[2 * which + (0 if is_mine else 1)]

                    @pl.when(jnp.logical_and(idx == pos, (core == half) == is_mine))
                    def _(src=src, off=off, lo=lo, w=hi - lo):
                        pltpu.make_async_copy(src.at[:, pl.ds(lo, w)], buf.at[slot, :, pl.ds(off, w)], sem.at[slot]).start()
                off += hi - lo

    @pl.when(step == 0)
    def _():
        fetch(n, 0)

    @pl.when(step + 1 < pl.num_programs(0) * nn)
    def _():
        fetch(lax.rem(n + 1, nn), lax.rem(step + 1, 2))

    slot = lax.rem(step, 2)
    pltpu.make_async_copy(buf.at[slot], buf.at[slot], sem.at[slot]).wait()
    acc = dot(a_ref[...], buf[slot], 0, 0)
    rows = acc.shape[0]

    def store(refs):
        for ref in refs:
            flat = ref.reshape(rows * 8, HD)
            for h in range(8):
                flat[pl.ds(h, rows, stride=8), :] = acc[:, h * HD:(h + 1) * HD]

    if n_out == 1:
        store((fulls[0], sends[0]))
    else:
        for pos in range(n_out):
            @pl.when(n == pos)
            def _(pos=pos):
                store((fulls[pos], sends[pos]))


def grad_wx(x, srcs, plan, heads, core):
    tok, dm = x.shape
    bm = 768
    nm = dm // 2 // bm
    flat = [a for pair in srcs for a in pair]
    if len(heads) == 1:
        col = lambda n: n
    else:
        col = lambda n: 0
    return pl.pallas_call(
        functools.partial(grad_wx_kernel, plan, len(srcs), len(heads)),
        grid_spec=pltpu.PrefetchScalarGridSpec(
            num_scalar_prefetch=1, grid=(nm, len(plan)),
            in_specs=[pl.BlockSpec((tok, bm), lambda m, n, c: (0, c[0] * nm + m))]
            + [pl.BlockSpec(memory_space=pl.ANY)] * len(flat),
            out_specs=[pl.BlockSpec((bm, 8, HD), lambda m, n, c: (c[0] * nm + m, col(n), 0)) for _ in heads]
            + [pl.BlockSpec((bm, 8, HD), lambda m, n, c: (m, col(n), 0)) for _ in heads],
            scratch_shapes=[pltpu.VMEM((2, tok, 8 * HD), jnp.bfloat16), pltpu.SemaphoreType.DMA((2,))]),
        out_shape=[jax.ShapeDtypeStruct((dm, h, HD), jnp.float32) for h in heads]
        + [jax.ShapeDtypeStruct((dm // 2, h, HD), jnp.float32) for h in heads],
        compiler_params=BIG, cost_estimate=cost(tok * dm * 8 * HD * len(plan), 2 * tok * dm))(core, x, *flat)


def merge_kernel(core_ref, *refs):
    n = (len(refs) - 2) // 3
    for i in range(n + 1):
        refs[2 * n + 1 + i][...] = refs[n + i][...]


def merge(fulls, recvs, gathered, core):
    steps = 12
    n = len(fulls)

    def spec(a, mine):
        block = (a.shape[0] // steps,) + a.shape[1:]
        zeros = (0,) * (len(block) - 1)
        if mine:
            return pl.BlockSpec(block, lambda i, c: (i,) + zeros)
        return pl.BlockSpec(block, lambda i, c: ((1 - c[0]) * steps + i,) + zeros)

    return pl.pallas_call(
        merge_kernel,
        grid_spec=pltpu.PrefetchScalarGridSpec(
            num_scalar_prefetch=1, grid=(steps,),
            in_specs=[pl.BlockSpec(memory_space=pl.ANY)] * n + [spec(r, True) for r in recvs] + [spec(gathered, True)],
            out_specs=[spec(r, False) for r in recvs] + [spec(gathered, True)]),
        out_shape=[jax.ShapeDtypeStruct(f.shape, f.dtype) for f in fulls] + [jax.ShapeDtypeStruct(gathered.shape, gathered.dtype)],
        input_output_aliases={1 + i: i for i in range(n)},
        compiler_params=BIG, cost_estimate=cost(1e10, 10 ** 8), name='merge')(core, *fulls, *recvs, gathered)


def y_kernel(idx_ref, loc_ref, rem_ref, w_ref, x_ref, y_ref, acc):
    k = pl.program_id(0)
    per = pl.num_programs(0) // 2
    nb, s, _ = x_ref.shape
    tok = nb * s
    mine = k // per == idx_ref[0]
    part = dot(jnp.where(mine, loc_ref[...].reshape(tok, -1), rem_ref[...].reshape(tok, -1)), w_ref[...], 1, 0)

    @pl.when(k == 0)
    def _():
        acc[...] = part

    @pl.when(k > 0)
    def _():
        acc[...] += part

    @pl.when(k == 2 * per - 1)
    def _():
        for b in range(nb):
            y_ref[b] = (x_ref[b].astype(jnp.float32) + acc[b * s:(b + 1) * s]).astype(jnp.bfloat16)


def out_proj(idx, o, o_rem, wo, x):
    nb, s, dm = x.shape
    wide = 768
    per = o.shape[3] // wide
    whole = pl.BlockSpec((nb, s, dm), lambda k, i: (0, 0, 0))
    return pl.pallas_call(
        y_kernel,
        grid_spec=pltpu.PrefetchScalarGridSpec(
            num_scalar_prefetch=1, grid=(2 * per,),
            in_specs=[pl.BlockSpec((1, nb, s, wide), lambda k, i: (i[1], 0, 0, lax.rem(k, per))),
                      pl.BlockSpec((nb, s, wide), lambda k, i: (0, 0, lax.rem(k, per))),
                      pl.BlockSpec((wide, dm), lambda k, i: (k, 0)), whole],
            out_specs=whole, scratch_shapes=[pltpu.VMEM((nb * s, dm), jnp.float32)]),
        out_shape=jax.ShapeDtypeStruct(x.shape, jnp.bfloat16),
        compiler_params=BIG, cost_estimate=cost(2 * nb * s * dm * dm, 2 * dm * dm), name='out_proj')(idx, o, o_rem, wo, x)


def dx_kernel(plan, n_src, idx_ref, *refs):
    srcs = refs[:2 * n_src]
    w_ref, x_ref, dy_ref, g_ref, dx_ref, dg_ref, acc = refs[2 * n_src:]
    k = pl.program_id(0)
    nb, s, dm = x_ref.shape
    for pos, pieces in enumerate(plan):
        @pl.when(k == pos)
        def _(pos=pos, pieces=pieces):
            cols = []
            for half, which, lo, hi in pieces:
                loc, rem = srcs[2 * which], srcs[2 * which + 1]
                cols.append(jnp.where(idx_ref[0] == half, loc[0, :, :, lo:hi].reshape(nb * s, hi - lo),
                                      rem[0, :, :, lo:hi].reshape(nb * s, hi - lo)))
            part = dot(jnp.concatenate(cols, axis=1), w_ref[...], 1, 1)
            if pos == 0:
                acc[...] = part
            else:
                acc[...] += part

    @pl.when(k == len(plan) - 1)
    def _():
        gain = g_ref[...].astype(jnp.float32)
        total = jnp.zeros((1, dm), jnp.float32)
        for b in range(nb):
            x32 = x_ref[b].astype(jnp.float32)
            inv = lax.rsqrt(jnp.mean(x32 * x32, axis=-1, keepdims=True) + EPS)
            unit = x32 * inv
            d_norm = acc[b * s:(b + 1) * s]
            total = total + jnp.sum(d_norm * unit, axis=0, keepdims=True)
            e = d_norm * gain
            d_x = inv * (e - unit * jnp.mean(e * unit, axis=-1, keepdims=True))
            dx_ref[b] = (dy_ref[b].astype(jnp.float32) + d_x).astype(jnp.bfloat16)
        dg_ref[...] = total


def cut(spans, wide):
    plan, room = [], 0
    for half, which, lo, end in spans:
        while lo < end:
            if room == 0:
                plan.append([])
                room = wide
            hi = min(end, lo + room)
            plan[-1].append((half, which, lo, hi))
            room -= hi - lo
            lo = hi
    return plan


def grad_x(idx, srcs, plan, wide, wcat, x, dy, gain):
    nb, s, dm = x.shape
    flat = [a for pair in srcs for a in pair]
    whole = pl.BlockSpec((nb, s, dm), lambda k, i: (0, 0, 0))
    line = pl.BlockSpec((1, dm), lambda k, i: (0, 0))
    return pl.pallas_call(
        functools.partial(dx_kernel, plan, len(srcs)),
        grid_spec=pltpu.PrefetchScalarGridSpec(
            num_scalar_prefetch=1, grid=(len(plan),),
            in_specs=[pl.BlockSpec((1, nb, s, a.shape[3]), lambda k, i: (i[1], 0, 0, 0)) for a in flat]
            + [pl.BlockSpec((dm, wide), lambda k, i: (0, k)), whole, whole, line],
            out_specs=[whole, line], scratch_shapes=[pltpu.VMEM((nb * s, dm), jnp.float32)]),
        out_shape=[jax.ShapeDtypeStruct(x.shape, jnp.bfloat16), jax.ShapeDtypeStruct((1, dm), jnp.float32)],
        compiler_params=BIG, cost_estimate=cost(2 * nb * s * dm * wide * len(plan), 2 * dm * dm),
        name='grad_x')(idx, *flat, wcat, x, dy, gain)


def solution(mesh):
    n_dev = mesh.shape['cp']
    n_chips = n_dev // 2
    pair = [(d, d ^ 1) for d in range(n_dev)]
    by_core = [[2 * p + c for c in range(2) for p in range(n_chips)]]

    def compute(x_in, dy_in, norm_gain, w_q, w_k, w_v, w_o):
        me = lax.axis_index('cp')
        core = me % 2
        nb, s, dm = x_in.shape
        n_heads, kv_heads = w_q.shape[1], w_k.shape[1]
        group = n_heads // kv_heads
        kvh = kv_heads // 2
        qd = n_heads * HD
        tok = n_dev * nb * s
        core_arr = core[None].astype(jnp.int32)
        chip_arr = (me // 2)[None].astype(jnp.int32)
        idx = jnp.stack([core, me]).astype(jnp.int32)

        def swap(a):
            return lax.ppermute(a, 'cp', pair)

        x32 = x_in.astype(jnp.float32)
        inv = lax.rsqrt(jnp.mean(x32 * x32, axis=-1, keepdims=True) + EPS)
        xn = (x32 * inv * norm_gain.astype(jnp.float32)).astype(jnp.bfloat16)
        own = nb * s
        xn = xn.reshape(own, dm)
        dy = dy_in.reshape(own, dm)
        wo = w_o.reshape(qd, dm)
        fence = lax.optimization_barrier
        cut_row = own // 2

        def hop(a, bit):
            return lax.ppermute(a, 'cp', [(d, d ^ bit) for d in range(n_dev)])

        def block(bit):
            return me ^ bit

        xn_x, xn_y, xn_c = hop(xn, 2), hop(xn, 4), swap(xn)
        wcat, wh = relayout(w_q, w_k, w_v, core_arr)
        dy_c = swap(dy)
        wide_qkv = wh.shape[1]
        seen = proj([(xn,), (xn_c,)], wh, [block(0), block(1)], core, tok, wide_qkv, 0, [])
        xn_x, xn_y, seen = fence((xn_x, xn_y, seen))
        xn_d = hop(xn_x[:cut_row], 4), hop(xn_y[cut_row:], 2)
        xn_xc, xn_yc = swap(xn_x), swap(xn_y)
        done = proj([(dy,), (dy_c,)], wo, [block(0), block(1)], core, tok, qd // 2, 1, [])
        xn_xc, xn_yc, done, seen, dy = fence((xn_xc, xn_yc, done, seen, dy))
        dy_x, dy_y = hop(dy, 2), hop(dy, 4)
        beside = [block(2), block(3), block(4), block(5)]
        across = [block(6), block(7)]
        seen = proj([(xn_x,), (xn_xc,), (xn_y,), (xn_yc,)], wh, beside, core, tok, wide_qkv, 0, seen)
        xn_d, seen = fence((xn_d, seen))
        xn_dc = swap(xn_d[0]), swap(xn_d[1])
        qkv, xg = proj([xn_d, xn_dc], wh, across, core, tok, wide_qkv, 0, seen)
        qkv = qkv.reshape(n_dev, nb, s, -1)
        fwd = attn_fwd(qkv, kvh, group, 0, nb // 2, [])
        dy_x, dy_y, fwd = fence((dy_x, dy_y, fwd))
        dy_d = hop(dy_x[:cut_row], 4), hop(dy_y[cut_row:], 2)
        dy_xc, dy_yc = swap(dy_x), swap(dy_y)
        o, log2n = attn_fwd(qkv, kvh, group, nb // 2, nb - nb // 2, fwd)
        o_rem = swap(lax.dynamic_index_in_dim(o, me ^ 1, 0, keepdims=False))
        y_out = out_proj(idx, o, o_rem, wo, x_in)
        dy_d, dy_xc, dy_yc, done, y_out = fence((dy_d, dy_xc, dy_yc, done, y_out))
        dy_dc = swap(dy_d[0]), swap(dy_d[1])
        done = proj([(dy_x,), (dy_xc,), (dy_y,), (dy_yc,)], wo, beside, core, tok, qd // 2, 1, done)
        do, dyg = proj([dy_d, dy_dc], wo, across, core, tok, qd // 2, 1, done)
        do = do.reshape(n_dev, nb, s, -1)
        d_wo = lax.all_gather(grad_wo(o.reshape(tok, -1), dyg, chip_arr, n_chips), 'cp', axis_index_groups=by_core, tiled=True)
        most = kvh - 1
        first = attn_bwd(qkv, o, do, log2n, kvh, group, 0, most)
        first_rem = swap(first)
        second = attn_bwd(qkv, o, do, log2n, kvh, group, most, kvh - most)
        second_rem = swap(second)
        first_rem, second_rem, xg = lax.optimization_barrier((first_rem, second_rem, xg))
        pairs = [(first, first_rem), (second, second_rem)]
        flat = [(a.reshape(tok, -1), b.reshape(tok, -1)) for a, b in pairs]
        wide = kv_heads * HD

        def columns(lo, hi):
            spans = []
            for h in range(2):
                for j in range(kvh):
                    base = (j % most) * (group + 2) * HD
                    spans.append((h, j // most, base + lo * HD, base + hi * HD))
            return spans

        by_q, by_k, by_v = columns(0, group), columns(group, group + 1), columns(group + 1, group + 2)
        wq_full, wq_send = grad_wx(xg, flat, cut(by_q, wide), (n_heads,), core_arr)
        wq_send, xg = lax.optimization_barrier((wq_send, xg))
        wq_recv = swap(wq_send)
        wk_full, wv_full, wk_send, wv_send = grad_wx(
            xg, flat, cut(by_k + by_v, wide), (kv_heads, kv_heads), core_arr)
        wk_send, wv_send, x_late = lax.optimization_barrier((wk_send, wv_send, x_in))
        wk_recv, wv_recv = swap(wk_send), swap(wv_send)
        dx_out, d_gain = grad_x(idx, pairs, cut(by_q + by_k + by_v, wide), wide, wcat, x_late, dy_in, norm_gain[None])
        d_gain = d_gain[0]

        def add_from(bit, a):
            return a + lax.ppermute(a, 'cp', [(d, d ^ bit) for d in range(n_dev)])

        d_gain = add_from(2, add_from(1, d_gain))
        wq_recv, wk_recv, wv_recv, d_wo, dx_out = lax.optimization_barrier((wq_recv, wk_recv, wv_recv, d_wo, dx_out))
        d_wq, d_wk, d_wv, d_wo = merge((wq_full, wk_full, wv_full), (wq_recv, wk_recv, wv_recv), d_wo, core_arr)
        d_gain = add_from(4, d_gain)
        d_wo = d_wo.reshape(n_heads, HD, dm)
        return y_out, dx_out, d_gain, d_wq, d_wk, d_wv, d_wo

    act_spec = P('dp', 'cp', None)
    mat_spec = P(None, None, None)
    grad_spec = P('dp', None, None)
    return jax.shard_map(compute, mesh=mesh,
                         in_specs=(act_spec, act_spec, P(None), mat_spec, mat_spec, mat_spec, mat_spec),
                         out_specs=(act_spec, act_spec, P('dp'), grad_spec, grad_spec, grad_spec, grad_spec),
                         check_vma=False)
```

```python
import functools
import math

import jax
import jax.numpy as jnp
from jax import lax
from jax.experimental import pallas as pl
from jax.experimental.pallas import tpu as pltpu
from jax.sharding import PartitionSpec as P

EPS = 1e-6
HD = 128
LOG2E = math.log2(math.e)
NEG = -1e30
BIG = pltpu.CompilerParams(vmem_limit_bytes=60 * 1024 * 1024)


def dot(a, b, ca, cb):
    return lax.dot_general(a, b, (((ca,), (cb,)), ((), ())), preferred_element_type=jnp.float32)


def cost(flops, nbytes):
    return pl.CostEstimate(flops=int(flops), bytes_accessed=int(nbytes), transcendentals=0)


def relayout_kernel(core_ref, wq_ref, wk_ref, wv_ref, out_ref, half_ref, tmp):
    rows = wq_ref.shape[0]
    first = core_ref[0] == 0
    col, base = 0, 0
    for ref in (wq_ref, wk_ref, wv_ref):
        width = ref.shape[1] * HD
        start = col
        for g in range(ref.shape[1] // 8):
            tmp[...] = ref[:, 8 * g:8 * g + 8, :].astype(jnp.float32).reshape(rows * 8, HD)
            for h in range(8):
                out_ref[:, col:col + HD] = tmp[pl.ds(h, rows, stride=8), :].astype(jnp.bfloat16)
                col += HD
        half = width // 2
        half_ref[:, base:base + half] = jnp.where(first, out_ref[:, start:start + half], out_ref[:, start + half:start + width])
        base += half


def relayout(w_q, w_k, w_v, core):
    dm = w_q.shape[0]
    cols = (w_q.shape[1] + w_k.shape[1] + w_v.shape[1]) * HD
    rows = 256
    return pl.pallas_call(
        relayout_kernel,
        grid_spec=pltpu.PrefetchScalarGridSpec(
            num_scalar_prefetch=1, grid=(dm // rows,),
            in_specs=[pl.BlockSpec((rows, w.shape[1], HD), lambda i, c: (i, 0, 0)) for w in (w_q, w_k, w_v)],
            out_specs=[pl.BlockSpec((rows, cols), lambda i, c: (i, 0)), pl.BlockSpec((rows, cols // 2), lambda i, c: (i, 0))],
            scratch_shapes=[pltpu.VMEM((rows * 8, HD), jnp.float32)]),
        out_shape=[jax.ShapeDtypeStruct((dm, cols), jnp.bfloat16), jax.ShapeDtypeStruct((dm, cols // 2), jnp.bfloat16)],
        cost_estimate=cost(1e10, 4 * dm * cols), name='relayout')(core, w_q, w_k, w_v)


def near_kernel(cb, tbl_ref, a_ref, b_ref, w_ref, o_ref):
    m = pl.program_id(1)
    a = jnp.where(m == 0, a_ref[...], b_ref[...])
    o_ref[...] = dot(a, w_ref[...], 1, cb).astype(jnp.bfloat16)


def far_kernel(cb, tbl_ref, a_ref, w_ref, old_ref, o_ref):
    o_ref[...] = dot(a_ref[...], w_ref[...], 1, cb).astype(jnp.bfloat16)


def proj_specs(w, width, cb, row):
    bn = width // 2
    if cb == 0:
        return bn, pl.BlockSpec((w.shape[0], bn), lambda n, m, t: (0, n))
    return bn, pl.BlockSpec((bn, w.shape[1]), lambda n, m, t: (2 * t[row] + n, 0))


def proj_near(a, b, w, tbl, tok, width, cb, name):
    bm, dm = a.shape
    bn, w_spec = proj_specs(w, width, cb, 2)
    line = pl.BlockSpec((bm, dm), lambda n, m, t: (0, 0))
    return pl.pallas_call(
        functools.partial(near_kernel, cb),
        grid_spec=pltpu.PrefetchScalarGridSpec(
            num_scalar_prefetch=1, grid=(2, 2), in_specs=[line, line, w_spec],
            out_specs=pl.BlockSpec((bm, bn), lambda n, m, t: (t[m], n))),
        out_shape=jax.ShapeDtypeStruct((tok, width), jnp.bfloat16),
        compiler_params=BIG, cost_estimate=cost(4 * bm * dm * width, 2 * dm * width), name=name)(tbl, a, b, w)


def proj_far(a, w, old, tbl, bm, cb, name):
    tok, dm = a.shape
    width = old.shape[1]
    rest = tok // bm - 2
    bn, w_spec = proj_specs(w, width, cb, rest)
    return pl.pallas_call(
        functools.partial(far_kernel, cb),
        grid_spec=pltpu.PrefetchScalarGridSpec(
            num_scalar_prefetch=1, grid=(2, rest),
            in_specs=[pl.BlockSpec((bm, dm), lambda n, m, t: (t[m], 0)), w_spec, pl.BlockSpec(memory_space=pl.ANY)],
            out_specs=pl.BlockSpec((bm, bn), lambda n, m, t: (t[m], n))),
        out_shape=jax.ShapeDtypeStruct(old.shape, jnp.bfloat16), input_output_aliases={3: 0},
        compiler_params=BIG, cost_estimate=cost(2 * rest * bm * dm * width, 2 * tok * dm), name=name)(tbl, a, w, old)


def stack(ref, rb, nblk, rows, group):
    parts = [ref[rb * nblk:(rb + 1) * nblk, 0, :, g * HD:(g + 1) * HD].reshape(rows, HD) for g in range(group)]
    return jnp.concatenate(parts, axis=0)


def fwd_kernel(rows, q_ref, k_ref, v_ref, o_ref, l_ref):
    n, _, blk, width = q_ref.shape
    group, seq, nblk = width // HD, n * blk, rows // blk
    c2 = HD ** -0.5 * LOG2E
    k = k_ref[...].reshape(seq, HD)
    v = v_ref[...].reshape(seq, HD)
    tall = group * rows
    row = lax.broadcasted_iota(jnp.int32, (tall, rows), 0) % rows
    col = lax.broadcasted_iota(jnp.int32, (tall, rows), 1)
    visible = row >= col

    def score(rb):
        return dot(stack(q_ref, rb, nblk, rows, group), k[:(rb + 1) * rows], 1, 1)

    s_next = score(0)
    for rb in range(seq // rows):
        r0 = rb * rows
        s = s_next
        if rb + 1 < seq // rows:
            s_next = score(rb + 1)
        s_d = jnp.where(visible, s[:, r0:], NEG)
        m = jnp.max(s_d, axis=1, keepdims=True)
        if rb:
            m = jnp.maximum(m, jnp.max(s[:, :r0], axis=1, keepdims=True))
        m = m * c2
        p_d = jnp.exp2(s_d * c2 - m)
        l = jnp.sum(p_d, axis=1, keepdims=True)
        p = p_d.astype(jnp.bfloat16)
        if rb:
            p_o = jnp.exp2(s[:, :r0] * c2 - m)
            l = l + jnp.sum(p_o, axis=1, keepdims=True)
            p = jnp.concatenate([p_o.astype(jnp.bfloat16), p], axis=1)
        acc = dot(p, v[:r0 + rows], 1, 0)
        o = (acc / l).astype(jnp.bfloat16)
        log2n = jnp.broadcast_to(m + jnp.log2(l), (tall, 128))
        for g in range(group):
            for j in range(nblk):
                o_ref[rb * nblk + j, 0, :, g * HD:(g + 1) * HD] = o[g * rows + j * blk:g * rows + (j + 1) * blk]
            l_ref[0, g, :, r0:r0 + rows] = log2n[g * rows:(g + 1) * rows].T[0:1]


def attn_fwd(qkv, kvh, group):
    n, nb, s, _ = qkv.shape
    width = group * HD
    first = kvh * group
    return pl.pallas_call(
        functools.partial(fwd_kernel, 128), grid=(nb, kvh),
        in_specs=[pl.BlockSpec((n, 1, s, width), lambda b, h: (0, b, 0, h)),
                  pl.BlockSpec((n, 1, s, HD), lambda b, h: (0, b, 0, first + h)),
                  pl.BlockSpec((n, 1, s, HD), lambda b, h: (0, b, 0, first + kvh + h))],
        out_specs=[pl.BlockSpec((n, 1, s, width), lambda b, h: (0, b, 0, h)),
                   pl.BlockSpec((1, group, 1, n * s), lambda b, h: (b, h, 0, 0))],
        out_shape=[jax.ShapeDtypeStruct((n, nb, s, kvh * width), jnp.bfloat16),
                   jax.ShapeDtypeStruct((nb, kvh * group, 1, n * s), jnp.float32)],
        compiler_params=BIG, cost_estimate=cost(nb * kvh * group * 4 * (n * s) ** 2 * HD, 10 ** 7),
        name='attn_fwd')(qkv, qkv, qkv)


def bwd_kernel(rows, q_ref, k_ref, v_ref, o_ref, do_ref, l_ref, d_ref, dq_acc):
    n, _, blk, width = q_ref.shape
    group, seq, nblk = width // HD, n * blk, rows // blk
    scale = HD ** -0.5
    c2 = scale * LOG2E
    k = k_ref[...].reshape(seq, HD)
    v = v_ref[...].reshape(seq, HD)
    row = lax.broadcasted_iota(jnp.int32, (rows, rows), 0)
    col = lax.broadcasted_iota(jnp.int32, (rows, rows), 1)
    visible = row <= col
    qs, dos, deltas = [], [], []
    for g in range(group):
        cols = slice(g * HD, (g + 1) * HD)
        qs.append(q_ref[:, 0, :, cols].reshape(seq, HD))
        d_o = do_ref[:, 0, :, cols].reshape(seq, HD)
        o = o_ref[:, 0, :, cols].reshape(seq, HD)
        dos.append(d_o)
        dcol = jnp.sum(d_o.astype(jnp.float32) * o.astype(jnp.float32), axis=1, keepdims=True)
        deltas.append(jnp.broadcast_to(dcol, (seq, 128)).T[0:1])
    units = [(kb, g) for kb in range(seq // rows) for g in range(group)]

    def score(unit):
        k0, g = unit[0] * rows, unit[1]
        return dot(k[k0:k0 + rows], qs[g][k0:], 1, 1), dot(v[k0:k0 + rows], dos[g][k0:], 1, 1)

    following = score(units[0])
    for i, (kb, g) in enumerate(units):
        k0 = kb * rows
        s, dp = following
        if i + 1 < len(units):
            following = score(units[i + 1])
        p = jnp.exp2(s * c2 - l_ref[0, g][:, k0:])
        p_d = jnp.where(visible, p[:, :rows], 0.0)
        p = p_d if k0 + rows == seq else jnp.concatenate([p_d, p[:, rows:]], axis=1)
        ds = (p * (dp - deltas[g][:, k0:]) * scale).astype(jnp.bfloat16)
        dv_c = dot(p.astype(jnp.bfloat16), dos[g][k0:], 1, 0)
        dk_c = dot(ds, qs[g][k0:], 1, 0)
        dq_c = dot(ds, k[k0:k0 + rows], 0, 0)
        if kb == 0:
            dq_acc[g] = dq_c
        else:
            dq_acc[g, k0:] += dq_c
        dv_t, dk_t = (dv_c, dk_c) if g == 0 else (dv_t + dv_c, dk_t + dk_c)
        if g == group - 1:
            for j, total in enumerate((dk_t, dv_t)):
                cols = slice(width + j * HD, width + (j + 1) * HD)
                d_ref[kb * nblk:(kb + 1) * nblk, 0, :, cols] = total.astype(jnp.bfloat16).reshape(nblk, blk, HD)
    for g in range(group):
        d_ref[:, 0, :, g * HD:(g + 1) * HD] = dq_acc[g].astype(jnp.bfloat16).reshape(n, blk, HD)


def attn_bwd(qkv, o, do, log2n, kvh, group, h0, count):
    n, nb, s, _ = qkv.shape
    width = group * HD
    first = kvh * group
    q_in = pl.BlockSpec((n, 1, s, width), lambda b, h: (0, b, 0, h0 + h))
    out = width + 2 * HD
    return pl.pallas_call(
        functools.partial(bwd_kernel, 256), grid=(nb, count),
        in_specs=[q_in,
                  pl.BlockSpec((n, 1, s, HD), lambda b, h: (0, b, 0, first + h0 + h)),
                  pl.BlockSpec((n, 1, s, HD), lambda b, h: (0, b, 0, first + kvh + h0 + h)),
                  q_in, q_in,
                  pl.BlockSpec((1, group, 1, n * s), lambda b, h: (b, h0 + h, 0, 0))],
        out_specs=pl.BlockSpec((n, 1, s, out), lambda b, h: (0, b, 0, h)),
        out_shape=jax.ShapeDtypeStruct((n, nb, s, count * out), jnp.bfloat16),
        scratch_shapes=[pltpu.VMEM((group, n * s, HD), jnp.float32)],
        compiler_params=BIG, cost_estimate=cost(nb * count * group * 10 * (n * s) ** 2 * HD, 10 ** 7),
        name='attn_bwd')(qkv, qkv, qkv, o, do, log2n)


def grad_wo_kernel(chip_ref, a_ref, b_ref, out_ref):
    out_ref[...] = dot(a_ref[...], b_ref[...], 0, 0)


def grad_wo(o, dy, chip, n_chips):
    tok, half = o.shape
    dm = dy.shape[1]
    bm, bn = half // n_chips, 1024
    return pl.pallas_call(
        grad_wo_kernel,
        grid_spec=pltpu.PrefetchScalarGridSpec(
            num_scalar_prefetch=1, grid=(dm // bn,),
            in_specs=[pl.BlockSpec((tok, bm), lambda n, c: (0, c[0])), pl.BlockSpec((tok, bn), lambda n, c: (0, n))],
            out_specs=pl.BlockSpec((bm, bn), lambda n, c: (0, n))),
        out_shape=jax.ShapeDtypeStruct((bm, dm), jnp.float32),
        compiler_params=BIG, cost_estimate=cost(2 * tok * bm * dm, 2 * tok * dm), name='grad_wo')(chip, o, dy)


def grad_wx_kernel(plan, n_src, n_out, core_ref, a_ref, *refs):
    srcs, fulls = refs[:2 * n_src], refs[2 * n_src:2 * n_src + n_out]
    sends, (buf, sem) = refs[2 * n_src + n_out:2 * n_src + 2 * n_out], refs[2 * n_src + 2 * n_out:]
    core = core_ref[0]
    n, nn = pl.program_id(1), pl.num_programs(1)
    step = pl.program_id(0) * nn + n

    def fetch(idx, slot):
        for pos, pieces in enumerate(plan):
            off = 0
            for half, which, lo, hi in pieces:
                for is_mine in (True, False):
                    src = srcs[2 * which + (0 if is_mine else 1)]

                    @pl.when(jnp.logical_and(idx == pos, (core == half) == is_mine))
                    def _(src=src, off=off, lo=lo, w=hi - lo):
                        pltpu.make_async_copy(src.at[:, pl.ds(lo, w)], buf.at[slot, :, pl.ds(off, w)], sem.at[slot]).start()
                off += hi - lo

    @pl.when(step == 0)
    def _():
        fetch(n, 0)

    @pl.when(step + 1 < pl.num_programs(0) * nn)
    def _():
        fetch(lax.rem(n + 1, nn), lax.rem(step + 1, 2))

    slot = lax.rem(step, 2)
    pltpu.make_async_copy(buf.at[slot], buf.at[slot], sem.at[slot]).wait()
    acc = dot(a_ref[...], buf[slot], 0, 0)
    rows = acc.shape[0]

    def store(refs):
        for ref in refs:
            flat = ref.reshape(rows * 8, HD)
            for h in range(8):
                flat[pl.ds(h, rows, stride=8), :] = acc[:, h * HD:(h + 1) * HD]

    if n_out == 1:
        store((fulls[0], sends[0]))
    else:
        for pos in range(n_out):
            @pl.when(n == pos)
            def _(pos=pos):
                store((fulls[pos], sends[pos]))


def grad_wx(x, srcs, plan, heads, core, name):
    tok, dm = x.shape
    bm = 768
    nm = dm // 2 // bm
    flat = [a for pair in srcs for a in pair]
    if len(heads) == 1:
        col = lambda n: n
    else:
        col = lambda n: 0
    return pl.pallas_call(
        functools.partial(grad_wx_kernel, plan, len(srcs), len(heads)),
        grid_spec=pltpu.PrefetchScalarGridSpec(
            num_scalar_prefetch=1, grid=(nm, len(plan)),
            in_specs=[pl.BlockSpec((tok, bm), lambda m, n, c: (0, c[0] * nm + m))]
            + [pl.BlockSpec(memory_space=pl.ANY)] * len(flat),
            out_specs=[pl.BlockSpec((bm, 8, HD), lambda m, n, c: (c[0] * nm + m, col(n), 0)) for _ in heads]
            + [pl.BlockSpec((bm, 8, HD), lambda m, n, c: (m, col(n), 0)) for _ in heads],
            scratch_shapes=[pltpu.VMEM((2, tok, 8 * HD), jnp.bfloat16), pltpu.SemaphoreType.DMA((2,))]),
        out_shape=[jax.ShapeDtypeStruct((dm, h, HD), jnp.float32) for h in heads]
        + [jax.ShapeDtypeStruct((dm // 2, h, HD), jnp.float32) for h in heads],
        compiler_params=BIG, cost_estimate=cost(tok * dm * 8 * HD * len(plan), 2 * tok * dm), name=name)(core, x, *flat)


def merge_kernel(core_ref, *refs):
    n = len(refs) // 3
    for i in range(n):
        refs[2 * n + i][...] = refs[n + i][...]


def merge(fulls, recvs, core):
    steps = 12
    n = len(fulls)

    def spec(a, mine):
        block = (a.shape[0] // steps,) + a.shape[1:]
        zeros = (0,) * (len(block) - 1)
        if mine:
            return pl.BlockSpec(block, lambda i, c: (i,) + zeros)
        return pl.BlockSpec(block, lambda i, c: ((1 - c[0]) * steps + i,) + zeros)

    return pl.pallas_call(
        merge_kernel,
        grid_spec=pltpu.PrefetchScalarGridSpec(
            num_scalar_prefetch=1, grid=(steps,),
            in_specs=[pl.BlockSpec(memory_space=pl.ANY)] * n + [spec(r, True) for r in recvs],
            out_specs=[spec(r, False) for r in recvs]),
        out_shape=[jax.ShapeDtypeStruct(f.shape, f.dtype) for f in fulls],
        input_output_aliases={1 + i: i for i in range(n)},
        cost_estimate=cost(1e10, 10 ** 8), name='merge')(core, *fulls, *recvs)


def y_kernel(idx_ref, loc_ref, rem_ref, w_ref, x_ref, y_ref, lhs):
    nb, s, _ = x_ref.shape
    half = loc_ref.shape[3]

    @pl.when(pl.program_id(0) == 0)
    def _():
        first = idx_ref[0] == 0
        loc = loc_ref[...].reshape(nb * s, half)
        rem = rem_ref[...].reshape(nb * s, half)
        lhs[:, :half] = jnp.where(first, loc, rem)
        lhs[:, half:] = jnp.where(first, rem, loc)

    acc = dot(lhs[...], w_ref[...], 1, 0)
    for b in range(nb):
        y_ref[b] = (x_ref[b].astype(jnp.float32) + acc[b * s:(b + 1) * s]).astype(jnp.bfloat16)


def out_proj(idx, o, o_rem, wo, x):
    nb, s, dm = x.shape
    half = o.shape[3]
    wide = 512
    cols = pl.BlockSpec((nb, s, wide), lambda k, i: (0, 0, k))
    return pl.pallas_call(
        y_kernel,
        grid_spec=pltpu.PrefetchScalarGridSpec(
            num_scalar_prefetch=1, grid=(dm // wide,),
            in_specs=[pl.BlockSpec((1, nb, s, half), lambda k, i: (i[1], 0, 0, 0)),
                      pl.BlockSpec((nb, s, half), lambda k, i: (0, 0, 0)),
                      pl.BlockSpec((2 * half, wide), lambda k, i: (0, k)), cols],
            out_specs=cols, scratch_shapes=[pltpu.VMEM((nb * s, 2 * half), jnp.bfloat16)]),
        out_shape=jax.ShapeDtypeStruct(x.shape, jnp.bfloat16),
        compiler_params=BIG, cost_estimate=cost(2 * nb * s * dm * dm, 2 * dm * dm), name='out_proj')(idx, o, o_rem, wo, x)


def dx_kernel(spans, n_src, idx_ref, *refs):
    srcs = refs[:2 * n_src]
    w_ref, x_ref, dy_ref, g_ref, from_ref, dx_ref, dg_ref, to_ref, lhs, acc = refs[2 * n_src:]
    n = pl.program_id(0)
    wide = w_ref.shape[0]
    steps = acc.shape[1] // wide
    tok, s = acc.shape[0], x_ref.shape[1]

    @pl.when(n == 0)
    def _():
        at = 0
        for half, which, lo, hi in spans:
            loc, rem = srcs[2 * which], srcs[2 * which + 1]
            lhs[:, at:at + hi - lo] = jnp.where(idx_ref[0] == half, loc[0, :, :, lo:hi].reshape(tok, hi - lo),
                                                rem[0, :, :, lo:hi].reshape(tok, hi - lo))
            at += hi - lo

    @pl.when(n < steps)
    def _():
        acc[:, pl.ds(pl.multiple_of(n * wide, wide), wide)] = dot(lhs[...], w_ref[...], 1, 1)
        to_ref[...] = from_ref[...]

    @pl.when(n >= steps)
    def _():
        b = n - steps
        gain = g_ref[...].astype(jnp.float32)
        x32 = x_ref[0].astype(jnp.float32)
        inv = lax.rsqrt(jnp.mean(x32 * x32, axis=-1, keepdims=True) + EPS)
        unit = x32 * inv
        d_norm = acc[pl.ds(pl.multiple_of(b * s, s), s), :]
        part = jnp.sum(d_norm * unit, axis=0, keepdims=True)
        dg_ref[...] = jnp.where(b == 0, part, dg_ref[...] + part)
        e = d_norm * gain
        d_x = inv * (e - unit * jnp.mean(e * unit, axis=-1, keepdims=True))
        dx_ref[0] = (dy_ref[0].astype(jnp.float32) + d_x).astype(jnp.bfloat16)


def cut(spans, wide):
    plan, room = [], 0
    for half, which, lo, end in spans:
        while lo < end:
            if room == 0:
                plan.append([])
                room = wide
            hi = min(end, lo + room)
            plan[-1].append((half, which, lo, hi))
            room -= hi - lo
            lo = hi
    return plan


def grad_x(idx, srcs, spans, wcat, x, dy, gain, gathered):
    nb, s, dm = x.shape
    cols = wcat.shape[1]
    wide = 256
    steps = dm // wide
    rows = gathered.shape[0] // steps
    flat = [a for pair in srcs for a in pair]
    seq = pl.BlockSpec((1, s, dm), lambda k, i: (jnp.maximum(k - steps, 0), 0, 0))
    line = pl.BlockSpec((1, dm), lambda k, i: (0, 0))
    share = pl.BlockSpec((rows, gathered.shape[1]), lambda k, i: (jnp.minimum(k, steps - 1), 0))
    return pl.pallas_call(
        functools.partial(dx_kernel, spans, len(srcs)),
        grid_spec=pltpu.PrefetchScalarGridSpec(
            num_scalar_prefetch=1, grid=(steps + nb,),
            in_specs=[pl.BlockSpec((1, nb, s, a.shape[3]), lambda k, i: (i[1], 0, 0, 0)) for a in flat]
            + [pl.BlockSpec((wide, cols), lambda k, i: (jnp.minimum(k, steps - 1), 0)), seq, seq, line, share],
            out_specs=[seq, line, share],
            scratch_shapes=[pltpu.VMEM((nb * s, cols), jnp.bfloat16), pltpu.VMEM((nb * s, dm), jnp.float32)]),
        out_shape=[jax.ShapeDtypeStruct(x.shape, jnp.bfloat16), jax.ShapeDtypeStruct((1, dm), jnp.float32),
                   jax.ShapeDtypeStruct(gathered.shape, gathered.dtype)],
        compiler_params=BIG, cost_estimate=cost(2 * nb * s * dm * cols, 2 * dm * cols),
        name='grad_x')(idx, *flat, wcat, x, dy, gain, gathered)


def solution(mesh):
    n_dev = mesh.shape['cp']
    n_chips = n_dev // 2
    pair = [(d, d ^ 1) for d in range(n_dev)]
    by_core = [[2 * p + c for c in range(2) for p in range(n_chips)]]

    def device_fn(x_in, dy_in, norm_gain, w_q, w_k, w_v, w_o):
        me = lax.axis_index('cp')
        core = me % 2
        nb, s, dm = x_in.shape
        n_heads, kv_heads = w_q.shape[1], w_k.shape[1]
        group = n_heads // kv_heads
        kvh = kv_heads // 2
        qd = n_heads * HD
        tok = n_dev * nb * s
        core_arr = core[None].astype(jnp.int32)
        chip_arr = (me // 2)[None].astype(jnp.int32)
        idx = jnp.stack([core, me]).astype(jnp.int32)

        def swap(a):
            return lax.ppermute(a, 'cp', pair)

        x32 = x_in.astype(jnp.float32)
        inv = lax.rsqrt(jnp.mean(x32 * x32, axis=-1, keepdims=True) + EPS)
        xn = (x32 * inv * norm_gain.astype(jnp.float32)).astype(jnp.bfloat16)
        own = nb * s
        xn = xn.reshape(own, dm)
        dy = dy_in.reshape(own, dm)
        xg = lax.all_gather(xn, 'cp', tiled=True)
        dyg = lax.all_gather(dy, 'cp', tiled=True)
        wcat, wh = relayout(w_q, w_k, w_v, core_arr)
        wo = w_o.reshape(qd, dm)
        near = jnp.stack([me, me ^ 1, core]).astype(jnp.int32)
        chip = me // 2
        far = [2 * lax.rem(chip + 1 + j // 2, n_chips) + j % 2 for j in range(n_dev - 2)]
        far = jnp.stack(far + [core]).astype(jnp.int32)
        qkv = proj_near(xn, swap(xn), wh, near, tok, wh.shape[1], 0, 'near_qkv')
        do = proj_near(dy, swap(dy), wo, near, tok, qd // 2, 1, 'near_do')
        qkv, do, xg = lax.optimization_barrier((qkv, do, xg))
        qkv = proj_far(xg, wh, qkv, far, own, 0, 'far_qkv').reshape(n_dev, nb, s, -1)
        o, log2n = attn_fwd(qkv, kvh, group)
        o_rem = swap(lax.dynamic_index_in_dim(o, me ^ 1, 0, keepdims=False))
        y_out = out_proj(idx, o, o_rem, wo, x_in)
        dyg, o, y_out = lax.optimization_barrier((dyg, o, y_out))
        d_wo = lax.all_gather(grad_wo(o.reshape(tok, -1), dyg, chip_arr, n_chips), 'cp', axis_index_groups=by_core, tiled=True)
        do = proj_far(dyg, wo, do, far, own, 1, 'far_do').reshape(n_dev, nb, s, -1)
        most = kvh - 1
        first = attn_bwd(qkv, o, do, log2n, kvh, group, 0, most)
        first_rem = swap(first)
        second = attn_bwd(qkv, o, do, log2n, kvh, group, most, kvh - most)
        second_rem = swap(second)
        first_rem, second_rem, xg = lax.optimization_barrier((first_rem, second_rem, xg))
        pairs = [(first, first_rem), (second, second_rem)]
        flat = [(a.reshape(tok, -1), b.reshape(tok, -1)) for a, b in pairs]
        wide = kv_heads * HD

        def columns(lo, hi):
            spans = []
            for h in range(2):
                for j in range(kvh):
                    base = (j % most) * (group + 2) * HD
                    spans.append((h, j // most, base + lo * HD, base + hi * HD))
            return spans

        by_q, by_k, by_v = columns(0, group), columns(group, group + 1), columns(group + 1, group + 2)
        wq_full, wq_send = grad_wx(xg, flat, cut(by_q, wide), (n_heads,), core_arr, 'grad_wq')
        wq_send, xg = lax.optimization_barrier((wq_send, xg))
        wq_recv = swap(wq_send)
        wk_full, wv_full, wk_send, wv_send = grad_wx(
            xg, flat, cut(by_k + by_v, wide), (kv_heads, kv_heads), core_arr, 'grad_wkv')
        wk_send, wv_send, x_late = lax.optimization_barrier((wk_send, wv_send, x_in))
        wk_recv, wv_recv = swap(wk_send), swap(wv_send)
        dx_out, d_gain, d_wo = grad_x(idx, pairs, by_q + by_k + by_v, wcat, x_late, dy_in, norm_gain[None], d_wo)
        d_gain = d_gain[0]

        def add_from(bit, a):
            return a + lax.ppermute(a, 'cp', [(d, d ^ bit) for d in range(n_dev)])

        d_gain = add_from(2, add_from(1, d_gain))
        wq_recv, wk_recv, wv_recv, dx_out = lax.optimization_barrier((wq_recv, wk_recv, wv_recv, dx_out))
        d_wq, d_wk, d_wv = merge((wq_full, wk_full, wv_full), (wq_recv, wk_recv, wv_recv), core_arr)
        d_gain = add_from(4, d_gain)
        d_wo = d_wo.reshape(n_heads, HD, dm)
        return y_out, dx_out, d_gain, d_wq, d_wk, d_wv, d_wo

    act_spec = P('dp', 'cp', None)
    mat_spec = P(None, None, None)
    grad_spec = P('dp', None, None)
    return jax.shard_map(device_fn, mesh=mesh,
                         in_specs=(act_spec, act_spec, P(None), mat_spec, mat_spec, mat_spec, mat_spec),
                         out_specs=(act_spec, act_spec, P('dp'), grad_spec, grad_spec, grad_spec, grad_spec),
                         check_vma=False)
```

```python
import functools
import math

import jax
import jax.numpy as jnp
from jax import lax
from jax.experimental import pallas as pl
from jax.experimental.pallas import tpu as pltpu
from jax.sharding import PartitionSpec as P

EPS = 1e-6
HD = 128
LOG2E = math.log2(math.e)
NEG = -1e30
BIG = pltpu.CompilerParams(vmem_limit_bytes=60 * 1024 * 1024)


def dot(a, b, ca, cb):
    return lax.dot_general(a, b, (((ca,), (cb,)), ((), ())), preferred_element_type=jnp.float32)


def cost(flops, nbytes):
    return pl.CostEstimate(flops=int(flops), bytes_accessed=int(nbytes), transcendentals=0)


def relayout_kernel(core_ref, wq_ref, wk_ref, wv_ref, out_ref, half_ref, tmp):
    rows = wq_ref.shape[0]
    first = core_ref[0] == 0
    col, base = 0, 0
    for ref in (wq_ref, wk_ref, wv_ref):
        width = ref.shape[1] * HD
        start = col
        for g in range(ref.shape[1] // 8):
            tmp[...] = ref[:, 8 * g:8 * g + 8, :].astype(jnp.float32).reshape(rows * 8, HD)
            for h in range(8):
                out_ref[:, col:col + HD] = tmp[pl.ds(h, rows, stride=8), :].astype(jnp.bfloat16)
                col += HD
        half = width // 2
        half_ref[:, base:base + half] = jnp.where(first, out_ref[:, start:start + half], out_ref[:, start + half:start + width])
        base += half


def relayout(w_q, w_k, w_v, core):
    dm = w_q.shape[0]
    cols = (w_q.shape[1] + w_k.shape[1] + w_v.shape[1]) * HD
    rows = 256
    return pl.pallas_call(
        relayout_kernel,
        grid_spec=pltpu.PrefetchScalarGridSpec(
            num_scalar_prefetch=1, grid=(dm // rows,),
            in_specs=[pl.BlockSpec((rows, w.shape[1], HD), lambda i, c: (i, 0, 0)) for w in (w_q, w_k, w_v)],
            out_specs=[pl.BlockSpec((rows, cols), lambda i, c: (i, 0)), pl.BlockSpec((rows, cols // 2), lambda i, c: (i, 0))],
            scratch_shapes=[pltpu.VMEM((rows * 8, HD), jnp.float32)]),
        out_shape=[jax.ShapeDtypeStruct((dm, cols), jnp.bfloat16), jax.ShapeDtypeStruct((dm, cols // 2), jnp.bfloat16)],
        cost_estimate=cost(1e10, 4 * dm * cols), name='relayout')(core, w_q, w_k, w_v)


def near_kernel(cb, tbl_ref, a_ref, b_ref, w_ref, o_ref):
    m = pl.program_id(1)
    a = jnp.where(m == 0, a_ref[...], b_ref[...])
    o_ref[...] = dot(a, w_ref[...], 1, cb).astype(jnp.bfloat16)


def far_kernel(cb, tbl_ref, a_ref, w_ref, old_ref, o_ref):
    o_ref[...] = dot(a_ref[...], w_ref[...], 1, cb).astype(jnp.bfloat16)


def proj_specs(w, width, cb, row):
    bn = width // 2
    if cb == 0:
        return bn, pl.BlockSpec((w.shape[0], bn), lambda n, m, t: (0, n))
    return bn, pl.BlockSpec((bn, w.shape[1]), lambda n, m, t: (2 * t[row] + n, 0))


def proj_near(a, b, w, tbl, tok, width, cb, name):
    bm, dm = a.shape
    bn, w_spec = proj_specs(w, width, cb, 2)
    line = pl.BlockSpec((bm, dm), lambda n, m, t: (0, 0))
    return pl.pallas_call(
        functools.partial(near_kernel, cb),
        grid_spec=pltpu.PrefetchScalarGridSpec(
            num_scalar_prefetch=1, grid=(2, 2), in_specs=[line, line, w_spec],
            out_specs=pl.BlockSpec((bm, bn), lambda n, m, t: (t[m], n))),
        out_shape=jax.ShapeDtypeStruct((tok, width), jnp.bfloat16),
        compiler_params=BIG, cost_estimate=cost(4 * bm * dm * width, 2 * dm * width), name=name)(tbl, a, b, w)


def proj_far(a, w, old, tbl, bm, cb, name):
    tok, dm = a.shape
    width = old.shape[1]
    rest = tok // bm - 2
    bn, w_spec = proj_specs(w, width, cb, rest)
    return pl.pallas_call(
        functools.partial(far_kernel, cb),
        grid_spec=pltpu.PrefetchScalarGridSpec(
            num_scalar_prefetch=1, grid=(2, rest),
            in_specs=[pl.BlockSpec((bm, dm), lambda n, m, t: (t[m], 0)), w_spec, pl.BlockSpec(memory_space=pl.ANY)],
            out_specs=pl.BlockSpec((bm, bn), lambda n, m, t: (t[m], n))),
        out_shape=jax.ShapeDtypeStruct(old.shape, jnp.bfloat16), input_output_aliases={3: 0},
        compiler_params=BIG, cost_estimate=cost(2 * rest * bm * dm * width, 2 * tok * dm), name=name)(tbl, a, w, old)


def stack(ref, rb, nblk, rows, group):
    parts = [ref[rb * nblk:(rb + 1) * nblk, 0, :, g * HD:(g + 1) * HD].reshape(rows, HD) for g in range(group)]
    return jnp.concatenate(parts, axis=0)


def fwd_kernel(rows, q_ref, k_ref, v_ref, o_ref, l_ref):
    n, _, blk, width = q_ref.shape
    group, seq, nblk = width // HD, n * blk, rows // blk
    c2 = HD ** -0.5 * LOG2E
    k = k_ref[...].reshape(seq, HD)
    v = v_ref[...].reshape(seq, HD)
    tall = group * rows
    row = lax.broadcasted_iota(jnp.int32, (tall, rows), 0) % rows
    col = lax.broadcasted_iota(jnp.int32, (tall, rows), 1)
    visible = row >= col

    def score(rb):
        return dot(stack(q_ref, rb, nblk, rows, group), k[:(rb + 1) * rows], 1, 1)

    s_next = score(0)
    for rb in range(seq // rows):
        r0 = rb * rows
        s = s_next
        if rb + 1 < seq // rows:
            s_next = score(rb + 1)
        s_d = jnp.where(visible, s[:, r0:], NEG)
        m = jnp.max(s_d, axis=1, keepdims=True)
        if rb:
            m = jnp.maximum(m, jnp.max(s[:, :r0], axis=1, keepdims=True))
        m = m * c2
        p_d = jnp.exp2(s_d * c2 - m)
        l = jnp.sum(p_d, axis=1, keepdims=True)
        p = p_d.astype(jnp.bfloat16)
        if rb:
            p_o = jnp.exp2(s[:, :r0] * c2 - m)
            l = l + jnp.sum(p_o, axis=1, keepdims=True)
            p = jnp.concatenate([p_o.astype(jnp.bfloat16), p], axis=1)
        acc = dot(p, v[:r0 + rows], 1, 0)
        o = (acc / l).astype(jnp.bfloat16)
        log2n = jnp.broadcast_to(m + jnp.log2(l), (tall, 128))
        for g in range(group):
            for j in range(nblk):
                o_ref[rb * nblk + j, 0, :, g * HD:(g + 1) * HD] = o[g * rows + j * blk:g * rows + (j + 1) * blk]
            l_ref[0, g, :, r0:r0 + rows] = log2n[g * rows:(g + 1) * rows].T[0:1]


def attn_fwd(qkv, kvh, group):
    n, nb, s, _ = qkv.shape
    width = group * HD
    first = kvh * group
    return pl.pallas_call(
        functools.partial(fwd_kernel, 128), grid=(nb, kvh),
        in_specs=[pl.BlockSpec((n, 1, s, width), lambda b, h: (0, b, 0, h)),
                  pl.BlockSpec((n, 1, s, HD), lambda b, h: (0, b, 0, first + h)),
                  pl.BlockSpec((n, 1, s, HD), lambda b, h: (0, b, 0, first + kvh + h))],
        out_specs=[pl.BlockSpec((n, 1, s, width), lambda b, h: (0, b, 0, h)),
                   pl.BlockSpec((1, group, 1, n * s), lambda b, h: (b, h, 0, 0))],
        out_shape=[jax.ShapeDtypeStruct((n, nb, s, kvh * width), jnp.bfloat16),
                   jax.ShapeDtypeStruct((nb, kvh * group, 1, n * s), jnp.float32)],
        compiler_params=BIG, cost_estimate=cost(nb * kvh * group * 4 * (n * s) ** 2 * HD, 10 ** 7),
        name='attn_fwd')(qkv, qkv, qkv)


def bwd_kernel(rows, q_ref, k_ref, v_ref, o_ref, do_ref, l_ref, d_ref, dq_acc):
    n, _, blk, width = q_ref.shape
    group, seq, nblk = width // HD, n * blk, rows // blk
    scale = HD ** -0.5
    c2 = scale * LOG2E
    k = k_ref[...].reshape(seq, HD)
    v = v_ref[...].reshape(seq, HD)
    row = lax.broadcasted_iota(jnp.int32, (rows, rows), 0)
    col = lax.broadcasted_iota(jnp.int32, (rows, rows), 1)
    visible = row <= col
    qs, dos, deltas = [], [], []
    for g in range(group):
        cols = slice(g * HD, (g + 1) * HD)
        qs.append(q_ref[:, 0, :, cols].reshape(seq, HD))
        d_o = do_ref[:, 0, :, cols].reshape(seq, HD)
        o = o_ref[:, 0, :, cols].reshape(seq, HD)
        dos.append(d_o)
        dcol = jnp.sum(d_o.astype(jnp.float32) * o.astype(jnp.float32), axis=1, keepdims=True)
        deltas.append(jnp.broadcast_to(dcol, (seq, 128)).T[0:1])
    units = [(kb, g) for kb in range(seq // rows) for g in range(group)]

    def score(unit):
        k0, g = unit[0] * rows, unit[1]
        return dot(k[k0:k0 + rows], qs[g][k0:], 1, 1), dot(v[k0:k0 + rows], dos[g][k0:], 1, 1)

    following = score(units[0])
    for i, (kb, g) in enumerate(units):
        k0 = kb * rows
        s, dp = following
        if i + 1 < len(units):
            following = score(units[i + 1])
        p = jnp.exp2(s * c2 - l_ref[0, g][:, k0:])
        p_d = jnp.where(visible, p[:, :rows], 0.0)
        p = p_d if k0 + rows == seq else jnp.concatenate([p_d, p[:, rows:]], axis=1)
        ds = (p * (dp - deltas[g][:, k0:]) * scale).astype(jnp.bfloat16)
        dv_c = dot(p.astype(jnp.bfloat16), dos[g][k0:], 1, 0)
        dk_c = dot(ds, qs[g][k0:], 1, 0)
        dq_c = dot(ds, k[k0:k0 + rows], 0, 0)
        if kb == 0:
            dq_acc[g] = dq_c
        else:
            dq_acc[g, k0:] += dq_c
        dv_t, dk_t = (dv_c, dk_c) if g == 0 else (dv_t + dv_c, dk_t + dk_c)
        if g == group - 1:
            for j, total in enumerate((dk_t, dv_t)):
                cols = slice(width + j * HD, width + (j + 1) * HD)
                d_ref[kb * nblk:(kb + 1) * nblk, 0, :, cols] = total.astype(jnp.bfloat16).reshape(nblk, blk, HD)
    for g in range(group):
        d_ref[:, 0, :, g * HD:(g + 1) * HD] = dq_acc[g].astype(jnp.bfloat16).reshape(n, blk, HD)


def attn_bwd(qkv, o, do, log2n, kvh, group, h0, count):
    n, nb, s, _ = qkv.shape
    width = group * HD
    first = kvh * group
    q_in = pl.BlockSpec((n, 1, s, width), lambda b, h: (0, b, 0, h0 + h))
    out = width + 2 * HD
    return pl.pallas_call(
        functools.partial(bwd_kernel, 256), grid=(nb, count),
        in_specs=[q_in,
                  pl.BlockSpec((n, 1, s, HD), lambda b, h: (0, b, 0, first + h0 + h)),
                  pl.BlockSpec((n, 1, s, HD), lambda b, h: (0, b, 0, first + kvh + h0 + h)),
                  q_in, q_in,
                  pl.BlockSpec((1, group, 1, n * s), lambda b, h: (b, h0 + h, 0, 0))],
        out_specs=pl.BlockSpec((n, 1, s, out), lambda b, h: (0, b, 0, h)),
        out_shape=jax.ShapeDtypeStruct((n, nb, s, count * out), jnp.bfloat16),
        scratch_shapes=[pltpu.VMEM((group, n * s, HD), jnp.float32)],
        compiler_params=BIG, cost_estimate=cost(nb * count * group * 10 * (n * s) ** 2 * HD, 10 ** 7),
        name='attn_bwd')(qkv, qkv, qkv, o, do, log2n)


def grad_wo_kernel(chip_ref, a_ref, b_ref, out_ref):
    out_ref[...] = dot(a_ref[...], b_ref[...], 0, 0)


def grad_wo(o, dy, chip, n_chips):
    tok, half = o.shape
    dm = dy.shape[1]
    bm, bn = half // n_chips, 1024
    return pl.pallas_call(
        grad_wo_kernel,
        grid_spec=pltpu.PrefetchScalarGridSpec(
            num_scalar_prefetch=1, grid=(dm // bn,),
            in_specs=[pl.BlockSpec((tok, bm), lambda n, c: (0, c[0])), pl.BlockSpec((tok, bn), lambda n, c: (0, n))],
            out_specs=pl.BlockSpec((bm, bn), lambda n, c: (0, n))),
        out_shape=jax.ShapeDtypeStruct((bm, dm), jnp.float32),
        compiler_params=BIG, cost_estimate=cost(2 * tok * bm * dm, 2 * tok * dm), name='grad_wo')(chip, o, dy)


def grad_wx_kernel(plan, n_src, n_out, core_ref, a_ref, *refs):
    srcs, fulls = refs[:2 * n_src], refs[2 * n_src:2 * n_src + n_out]
    sends, (buf, sem) = refs[2 * n_src + n_out:2 * n_src + 2 * n_out], refs[2 * n_src + 2 * n_out:]
    core = core_ref[0]
    n, nn = pl.program_id(1), pl.num_programs(1)
    step = pl.program_id(0) * nn + n

    def fetch(idx, slot):
        for pos, pieces in enumerate(plan):
            off = 0
            for half, which, lo, hi in pieces:
                for is_mine in (True, False):
                    src = srcs[2 * which + (0 if is_mine else 1)]

                    @pl.when(jnp.logical_and(idx == pos, (core == half) == is_mine))
                    def _(src=src, off=off, lo=lo, w=hi - lo):
                        pltpu.make_async_copy(src.at[:, pl.ds(lo, w)], buf.at[slot, :, pl.ds(off, w)], sem.at[slot]).start()
                off += hi - lo

    keep = len(plan) == 2
    slot = lax.rem(step, 2)

    @pl.when(step == 0)
    def _():
        fetch(n, 0)

    @pl.when(step + 1 < (nn if keep else pl.num_programs(0) * nn))
    def _():
        fetch(lax.rem(n + 1, nn), lax.rem(step + 1, 2))

    @pl.when(step < (nn if keep else pl.num_programs(0) * nn))
    def _():
        pltpu.make_async_copy(buf.at[slot], buf.at[slot], sem.at[slot]).wait()

    acc = dot(a_ref[...], buf[slot], 0, 0)
    rows = acc.shape[0]

    def store(refs):
        for ref in refs:
            flat = ref.reshape(rows * 8, HD)
            for h in range(8):
                flat[pl.ds(h, rows, stride=8), :] = acc[:, h * HD:(h + 1) * HD]

    if n_out == 1:
        store((fulls[0], sends[0]))
    else:
        for pos in range(n_out):
            @pl.when(n == pos)
            def _(pos=pos):
                store((fulls[pos], sends[pos]))


def grad_wx(x, srcs, plan, heads, core, name):
    tok, dm = x.shape
    bm = 768
    nm = dm // 2 // bm
    flat = [a for pair in srcs for a in pair]
    if len(heads) == 1:
        col = lambda n: n
    else:
        col = lambda n: 0
    return pl.pallas_call(
        functools.partial(grad_wx_kernel, plan, len(srcs), len(heads)),
        grid_spec=pltpu.PrefetchScalarGridSpec(
            num_scalar_prefetch=1, grid=(nm, len(plan)),
            in_specs=[pl.BlockSpec((tok, bm), lambda m, n, c: (0, c[0] * nm + m))]
            + [pl.BlockSpec(memory_space=pl.ANY)] * len(flat),
            out_specs=[pl.BlockSpec((bm, 8, HD), lambda m, n, c: (c[0] * nm + m, col(n), 0)) for _ in heads]
            + [pl.BlockSpec((bm, 8, HD), lambda m, n, c: (m, col(n), 0)) for _ in heads],
            scratch_shapes=[pltpu.VMEM((2, tok, 8 * HD), jnp.bfloat16), pltpu.SemaphoreType.DMA((2,))]),
        out_shape=[jax.ShapeDtypeStruct((dm, h, HD), jnp.float32) for h in heads]
        + [jax.ShapeDtypeStruct((dm // 2, h, HD), jnp.float32) for h in heads],
        compiler_params=BIG, cost_estimate=cost(tok * dm * 8 * HD * len(plan), 2 * tok * dm), name=name)(core, x, *flat)


def merge_kernel(core_ref, *refs):
    n = (len(refs) - 2) // 3
    for i in range(n + 1):
        refs[2 * n + 1 + i][...] = refs[n + i][...]


def merge(fulls, recvs, gathered, core):
    steps = 12
    n = len(fulls)

    def spec(a, mine):
        block = (a.shape[0] // steps,) + a.shape[1:]
        zeros = (0,) * (len(block) - 1)
        if mine:
            return pl.BlockSpec(block, lambda i, c: (i,) + zeros)
        return pl.BlockSpec(block, lambda i, c: ((1 - c[0]) * steps + i,) + zeros)

    return pl.pallas_call(
        merge_kernel,
        grid_spec=pltpu.PrefetchScalarGridSpec(
            num_scalar_prefetch=1, grid=(steps,),
            in_specs=[pl.BlockSpec(memory_space=pl.ANY)] * n + [spec(r, True) for r in recvs] + [spec(gathered, True)],
            out_specs=[spec(r, False) for r in recvs] + [spec(gathered, True)]),
        out_shape=[jax.ShapeDtypeStruct(f.shape, f.dtype) for f in fulls] + [jax.ShapeDtypeStruct(gathered.shape, gathered.dtype)],
        input_output_aliases={1 + i: i for i in range(n)},
        compiler_params=BIG, cost_estimate=cost(1e10, 10 ** 8), name='merge')(core, *fulls, *recvs, gathered)


def y_kernel(idx_ref, loc_ref, rem_ref, w_ref, x_ref, y_ref, lhs):
    nb, s, _ = x_ref.shape
    half = loc_ref.shape[3]

    @pl.when(pl.program_id(0) == 0)
    def _():
        first = idx_ref[0] == 0
        loc = loc_ref[...].reshape(nb * s, half)
        rem = rem_ref[...].reshape(nb * s, half)
        lhs[:, :half] = jnp.where(first, loc, rem)
        lhs[:, half:] = jnp.where(first, rem, loc)

    acc = dot(lhs[...], w_ref[...], 1, 0)
    for b in range(nb):
        y_ref[b] = (x_ref[b].astype(jnp.float32) + acc[b * s:(b + 1) * s]).astype(jnp.bfloat16)


def out_proj(idx, o, o_rem, wo, x):
    nb, s, dm = x.shape
    half = o.shape[3]
    wide = 512
    cols = pl.BlockSpec((nb, s, wide), lambda k, i: (0, 0, k))
    return pl.pallas_call(
        y_kernel,
        grid_spec=pltpu.PrefetchScalarGridSpec(
            num_scalar_prefetch=1, grid=(dm // wide,),
            in_specs=[pl.BlockSpec((1, nb, s, half), lambda k, i: (i[1], 0, 0, 0)),
                      pl.BlockSpec((nb, s, half), lambda k, i: (0, 0, 0)),
                      pl.BlockSpec((2 * half, wide), lambda k, i: (0, k)), cols],
            out_specs=cols, scratch_shapes=[pltpu.VMEM((nb * s, 2 * half), jnp.bfloat16)]),
        out_shape=jax.ShapeDtypeStruct(x.shape, jnp.bfloat16),
        compiler_params=BIG, cost_estimate=cost(2 * nb * s * dm * dm, 2 * dm * dm), name='out_proj')(idx, o, o_rem, wo, x)


def dx_kernel(spans, n_src, idx_ref, *refs):
    srcs = refs[:2 * n_src]
    w_ref, x_ref, dy_ref, g_ref, dx_ref, dg_ref, lhs, acc = refs[2 * n_src:]
    n = pl.program_id(0)
    wide = w_ref.shape[0]
    steps = acc.shape[1] // wide
    tok, s = acc.shape[0], x_ref.shape[1]

    @pl.when(n == 0)
    def _():
        at = 0
        for half, which, lo, hi in spans:
            loc, rem = srcs[2 * which], srcs[2 * which + 1]
            lhs[:, at:at + hi - lo] = jnp.where(idx_ref[0] == half, loc[0, :, :, lo:hi].reshape(tok, hi - lo),
                                                rem[0, :, :, lo:hi].reshape(tok, hi - lo))
            at += hi - lo

    @pl.when(n < steps)
    def _():
        acc[:, pl.ds(pl.multiple_of(n * wide, wide), wide)] = dot(lhs[...], w_ref[...], 1, 1)

    @pl.when(n >= steps)
    def _():
        b = n - steps
        gain = g_ref[...].astype(jnp.float32)
        x32 = x_ref[0].astype(jnp.float32)
        inv = lax.rsqrt(jnp.mean(x32 * x32, axis=-1, keepdims=True) + EPS)
        unit = x32 * inv
        d_norm = acc[pl.ds(pl.multiple_of(b * s, s), s), :]
        part = jnp.sum(d_norm * unit, axis=0, keepdims=True)
        dg_ref[...] = jnp.where(b == 0, part, dg_ref[...] + part)
        e = d_norm * gain
        d_x = inv * (e - unit * jnp.mean(e * unit, axis=-1, keepdims=True))
        dx_ref[0] = (dy_ref[0].astype(jnp.float32) + d_x).astype(jnp.bfloat16)


def cut(spans, wide):
    plan, room = [], 0
    for half, which, lo, end in spans:
        while lo < end:
            if room == 0:
                plan.append([])
                room = wide
            hi = min(end, lo + room)
            plan[-1].append((half, which, lo, hi))
            room -= hi - lo
            lo = hi
    return plan


def grad_x(idx, srcs, spans, wcat, x, dy, gain):
    nb, s, dm = x.shape
    cols = wcat.shape[1]
    wide = 512
    steps = dm // wide
    flat = [a for pair in srcs for a in pair]
    seq = pl.BlockSpec((1, s, dm), lambda k, i: (jnp.maximum(k - steps, 0), 0, 0))
    line = pl.BlockSpec((1, dm), lambda k, i: (0, 0))
    return pl.pallas_call(
        functools.partial(dx_kernel, spans, len(srcs)),
        grid_spec=pltpu.PrefetchScalarGridSpec(
            num_scalar_prefetch=1, grid=(steps + nb,),
            in_specs=[pl.BlockSpec((1, nb, s, a.shape[3]), lambda k, i: (i[1], 0, 0, 0)) for a in flat]
            + [pl.BlockSpec((wide, cols), lambda k, i: (jnp.minimum(k, steps - 1), 0)), seq, seq, line],
            out_specs=[seq, line],
            scratch_shapes=[pltpu.VMEM((nb * s, cols), jnp.bfloat16), pltpu.VMEM((nb * s, dm), jnp.float32)]),
        out_shape=[jax.ShapeDtypeStruct(x.shape, jnp.bfloat16), jax.ShapeDtypeStruct((1, dm), jnp.float32)],
        compiler_params=BIG, cost_estimate=cost(2 * nb * s * dm * cols, 2 * dm * cols),
        name='grad_x')(idx, *flat, wcat, x, dy, gain)


def solution(mesh):
    n_dev = mesh.shape['cp']
    n_chips = n_dev // 2
    pair = [(d, d ^ 1) for d in range(n_dev)]
    by_core = [[2 * p + c for c in range(2) for p in range(n_chips)]]

    def device_fn(x_in, dy_in, norm_gain, w_q, w_k, w_v, w_o):
        me = lax.axis_index('cp')
        core = me % 2
        nb, s, dm = x_in.shape
        n_heads, kv_heads = w_q.shape[1], w_k.shape[1]
        group = n_heads // kv_heads
        kvh = kv_heads // 2
        qd = n_heads * HD
        tok = n_dev * nb * s
        core_arr = core[None].astype(jnp.int32)
        chip_arr = (me // 2)[None].astype(jnp.int32)
        idx = jnp.stack([core, me]).astype(jnp.int32)

        def swap(a):
            return lax.ppermute(a, 'cp', pair)

        x32 = x_in.astype(jnp.float32)
        inv = lax.rsqrt(jnp.mean(x32 * x32, axis=-1, keepdims=True) + EPS)
        xn = (x32 * inv * norm_gain.astype(jnp.float32)).astype(jnp.bfloat16)
        own = nb * s
        xn = xn.reshape(own, dm)
        dy = dy_in.reshape(own, dm)
        xg = lax.all_gather(xn, 'cp', tiled=True)
        dyg = lax.all_gather(dy, 'cp', tiled=True)
        wcat, wh = relayout(w_q, w_k, w_v, core_arr)
        wo = w_o.reshape(qd, dm)
        near = jnp.stack([me, me ^ 1, core]).astype(jnp.int32)
        chip = me // 2
        far = [2 * lax.rem(chip + 1 + j // 2, n_chips) + j % 2 for j in range(n_dev - 2)]
        far = jnp.stack(far + [core]).astype(jnp.int32)
        qkv = proj_near(xn, swap(xn), wh, near, tok, wh.shape[1], 0, 'near_qkv')
        do = proj_near(dy, swap(dy), wo, near, tok, qd // 2, 1, 'near_do')
        qkv, do, xg = lax.optimization_barrier((qkv, do, xg))
        qkv = proj_far(xg, wh, qkv, far, own, 0, 'far_qkv').reshape(n_dev, nb, s, -1)
        o, log2n = attn_fwd(qkv, kvh, group)
        o_rem = swap(lax.dynamic_index_in_dim(o, me ^ 1, 0, keepdims=False))
        y_out = out_proj(idx, o, o_rem, wo, x_in)
        dyg, o, y_out = lax.optimization_barrier((dyg, o, y_out))
        d_wo = lax.all_gather(grad_wo(o.reshape(tok, -1), dyg, chip_arr, n_chips), 'cp', axis_index_groups=by_core, tiled=True)
        do = proj_far(dyg, wo, do, far, own, 1, 'far_do').reshape(n_dev, nb, s, -1)
        most = kvh - 1
        first = attn_bwd(qkv, o, do, log2n, kvh, group, 0, most)
        first_rem = swap(first)
        second = attn_bwd(qkv, o, do, log2n, kvh, group, most, kvh - most)
        second_rem = swap(second)
        first_rem, second_rem, xg = lax.optimization_barrier((first_rem, second_rem, xg))
        pairs = [(first, first_rem), (second, second_rem)]
        flat = [(a.reshape(tok, -1), b.reshape(tok, -1)) for a, b in pairs]
        wide = kv_heads * HD

        def columns(lo, hi):
            spans = []
            for h in range(2):
                for j in range(kvh):
                    base = (j % most) * (group + 2) * HD
                    spans.append((h, j // most, base + lo * HD, base + hi * HD))
            return spans

        by_q, by_k, by_v = columns(0, group), columns(group, group + 1), columns(group + 1, group + 2)
        wq_full, wq_send = grad_wx(xg, flat, cut(by_q, wide), (n_heads,), core_arr, 'grad_wq')
        wq_send, xg = lax.optimization_barrier((wq_send, xg))
        wq_recv = swap(wq_send)
        wk_full, wv_full, wk_send, wv_send = grad_wx(
            xg, flat, cut(by_k + by_v, wide), (kv_heads, kv_heads), core_arr, 'grad_wkv')
        wk_send, wv_send, x_late = lax.optimization_barrier((wk_send, wv_send, x_in))
        wk_recv, wv_recv = swap(wk_send), swap(wv_send)
        dx_out, d_gain = grad_x(idx, pairs, by_q + by_k + by_v, wcat, x_late, dy_in, norm_gain[None])
        d_gain = d_gain[0]

        def add_from(bit, a):
            return a + lax.ppermute(a, 'cp', [(d, d ^ bit) for d in range(n_dev)])

        d_gain = add_from(2, add_from(1, d_gain))
        wq_recv, wk_recv, wv_recv, d_wo, dx_out = lax.optimization_barrier((wq_recv, wk_recv, wv_recv, d_wo, dx_out))
        d_wq, d_wk, d_wv, d_wo = merge((wq_full, wk_full, wv_full), (wq_recv, wk_recv, wv_recv), d_wo, core_arr)
        d_gain = add_from(4, d_gain)
        d_wo = d_wo.reshape(n_heads, HD, dm)
        return y_out, dx_out, d_gain, d_wq, d_wk, d_wv, d_wo

    act_spec = P('dp', 'cp', None)
    mat_spec = P(None, None, None)
    grad_spec = P('dp', None, None)
    return jax.shard_map(device_fn, mesh=mesh,
                         in_specs=(act_spec, act_spec, P(None), mat_spec, mat_spec, mat_spec, mat_spec),
                         out_specs=(act_spec, act_spec, P('dp'), grad_spec, grad_spec, grad_spec, grad_spec),
                         check_vma=False)
```
